256 devices in a mesh: groups: 4 (over x, y), seq: 64 (over z, core).
Axes of the slice: x: 2, y: 2, z: 32, core: 2. Of those that a mesh axis runs over, the one named last changes fastest.
The devices are a block of a 4x8x32 slice.
Arguments:
- video_qkv: bfloat16 [16, 16, 3, 3072, 128], P('groups', None, None, 'seq'), parts along dimension 0, may hold values from -9 to 9
- video_cross: bfloat16 [16, 16, 3, 3072, 128], P('groups', None, None, 'seq'), parts along dimension 0, may hold values from -9 to 9
- audio_qkv: bfloat16 [16, 16, 3, 768, 128], P('groups', None, None, 'seq'), parts along dimension 0, may hold values from -9 to 9
- audio_cross: bfloat16 [16, 16, 3, 768, 128], P('groups', None, None, 'seq'), parts along dimension 0, may hold values from -9 to 9
- lengths: int32 [2, 16], P(None, 'groups'), parts along dimension 1, may hold values from 384 to 3072, as said below
- timestep: int32 [4], P('groups'), parts along dimension 0, may hold values from 0 to 49
- gate_table: float32 [50, 4, 16, 128], replicated, may hold values from -4 to 4
Outputs:
- video_out: bfloat16 [16, 16, 3072, 128], P('groups', None, 'seq'), parts along dimension 0
- audio_out: bfloat16 [16, 16, 768, 128], P('groups', None, 'seq'), parts along dimension 0
The draws below stay inside these ranges and needn't reach their ends.
There are 4 independent parts, one for each index of `groups`. The reference program is written for one: setup_inputs(seed, part) draws one part's arguments, and reference() takes and returns one part's arrays. A program takes and returns all parts, laid end to end along the dimension named above; an argument that names none is the same for every part. Nothing has to cross between parts.
Inputs may be any that keep to these rules, and one draw needn't show every extreme that they name: `lengths`: row 0 holds each clip's valid video token count, row 1 its valid audio token count; every count is at least half of its tower's length (3072 or 768), and in every draw some clip has all 3072 video tokens and some clip all 768 audio tokens valid.
All inputs are finite; a program needn't handle non-finite values.
Results may differ from the reference program's by a relative error of at most 0.0085.
Values may be sent and summed in bfloat16 or wider, within the bound.
A program may use at most 64 MiB of HBM per device.

```python
import math
import jax
import jax.numpy as jnp
from jax import lax

HEADS = 16
HEADDIM = 128
SEQS = 4
LV = 3072
LA = 768
STEPS = 50


def noise_block(key, length):
    subkeys = jax.random.split(key, 3)
    block_shape = (SEQS, HEADS, length, HEADDIM)
    query_part = jnp.clip(1.5 * jax.random.normal(subkeys[0], block_shape, jnp.float32), -9.0, 9.0)
    key_part = jnp.clip(1.5 * jax.random.normal(subkeys[1], block_shape, jnp.float32), -9.0, 9.0)
    value_part = jnp.clip(jax.random.normal(subkeys[2], block_shape, jnp.float32), -9.0, 9.0)
    return (query_part, key_part, value_part)


def stacked(query_part, key_part, value_part):
    return jnp.stack([query_part, key_part, value_part], axis=2).astype(jnp.bfloat16)


def draw_video_qkv(key, part):
    query_part, key_part, value_part = noise_block(jax.random.fold_in(key, 11), LV)
    return stacked(query_part, key_part, value_part)


def draw_audio_qkv(key, part):
    query_part, key_part, value_part = noise_block(jax.random.fold_in(key, 13), LA)
    return stacked(query_part, key_part, value_part)


def draw_video_cross(key, part):
    query_part, key_part, value_part = noise_block(jax.random.fold_in(key, 12), LV)
    return stacked(query_part, key_part, value_part)


def draw_audio_cross(key, part):
    query_part, key_part, value_part = noise_block(jax.random.fold_in(key, 14), LA)
    return stacked(query_part, key_part, value_part)


def draw_lengths(key, part):
    subkeys = jax.random.split(jax.random.fold_in(key, 31), 4)
    video_count = jax.random.randint(subkeys[0], (SEQS,), LV // 2, LV + 1)
    audio_count = jax.random.randint(subkeys[1], (SEQS,), LA // 2, LA + 1)
    full_video = jax.random.randint(subkeys[2], (), 0, SEQS)
    full_audio = jax.random.randint(subkeys[3], (), 0, SEQS)
    clip_index = jnp.arange(SEQS)
    video_count = jnp.where(clip_index == full_video, LV, video_count)
    audio_count = jnp.where(clip_index == full_audio, LA, audio_count)
    return jnp.stack([video_count, audio_count]).astype(jnp.int32)


def noise(own_key, extent, spread, bound, held_as=jnp.bfloat16):
    return jnp.clip(spread * jax.random.normal(own_key, extent, jnp.float32), -bound, bound).astype(held_as)


def setup_inputs(seed: int = 0, part: int = 0) -> dict:
    streams_of = jax.random.split(jax.random.key(seed), 8)
    part_splits = jax.random.split(jax.random.fold_in(streams_of[7], part), 8)
    return {
        "video_qkv": draw_video_qkv(jax.random.fold_in(jax.random.fold_in(streams_of[7], part), 71), part),
        "video_cross": draw_video_cross(jax.random.fold_in(jax.random.fold_in(streams_of[7], part), 71), part),
        "audio_qkv": draw_audio_qkv(jax.random.fold_in(jax.random.fold_in(streams_of[7], part), 71), part),
        "audio_cross": draw_audio_cross(jax.random.fold_in(jax.random.fold_in(streams_of[7], part), 71), part),
        "lengths": draw_lengths(jax.random.fold_in(jax.random.fold_in(streams_of[7], part), 71), part),
        "timestep": jax.random.randint(part_splits[5], (1,), 0, STEPS).astype(jnp.int32),
        "gate_table": noise(streams_of[6], (STEPS, 4, HEADS, HEADDIM), 1.0, 4.0, jnp.float32),
    }


def attend(queries, key_rows, values, keep_len):
    row_count = queries.shape[0]
    block_rows = row_count if row_count <= 1024 else math.gcd(row_count, 1024)
    score_scale = 1.0 / math.sqrt(queries.shape[1])
    columns = jnp.arange(key_rows.shape[0], dtype=jnp.int32)
    visible = columns[None, :] < keep_len
    blocks = queries.reshape(row_count // block_rows, block_rows, queries.shape[1])

    def one_block(query_block):
        scores = lax.dot_general(query_block, key_rows, (((1,), (1,)), ((), ())), preferred_element_type=jnp.float32) * score_scale
        scores = jnp.where(visible, scores, -1e+30)
        row_max = lax.optimization_barrier(jnp.max(scores, axis=1, keepdims=True))
        weights = jnp.exp(scores - row_max)
        row_total = lax.optimization_barrier(jnp.sum(weights, axis=1, keepdims=True))
        shares = (weights / row_total).astype(jnp.bfloat16)
        return jnp.dot(shares, values, preferred_element_type=jnp.float32).astype(jnp.bfloat16)
    return lax.map(one_block, blocks).reshape(row_count, queries.shape[1])

def pair_outputs(bundle):
    video_set, video_far, audio_set, audio_far, video_len, audio_len = bundle
    self_video = attend(video_set[0], video_set[1], video_set[2], video_len)
    cross_video = attend(video_far[0], audio_far[1], audio_far[2], audio_len)
    self_audio = attend(audio_set[0], audio_set[1], audio_set[2], audio_len)
    cross_audio = attend(audio_far[0], video_far[1], video_far[2], video_len)
    return (self_video, cross_video, self_audio, cross_audio)

def combine(self_part, cross_part, gate_self, gate_cross, clip_count):
    head_count = gate_self.shape[0]
    shaped = (clip_count, head_count) + self_part.shape[1:]
    mixed_sum = gate_self[None, :, None, :] * self_part.reshape(shaped).astype(jnp.float32) + gate_cross[None, :, None, :] * cross_part.reshape(shaped).astype(jnp.float32)
    return mixed_sum.astype(jnp.bfloat16)

def reference(video_qkv, video_cross, audio_qkv, audio_cross, lengths, timestep, gate_table):
    clip_count, head_count = (video_qkv.shape[0], video_qkv.shape[1])
    pair_count = clip_count * head_count
    step_ids = jnp.arange(gate_table.shape[0], dtype=jnp.int32)
    gate_rows = lax.optimization_barrier(jnp.sum(jnp.where((step_ids == timestep[0])[:, None, None, None], gate_table, 0.0), axis=0))
    clip_ids = jnp.arange(pair_count, dtype=jnp.int32) // head_count
    video_lens = lengths[0][clip_ids].astype(jnp.int32)
    audio_lens = lengths[1][clip_ids].astype(jnp.int32)

    def to_pairs(tensor):
        return tensor.reshape((pair_count,) + tensor.shape[2:])
    self_video, cross_video, self_audio, cross_audio = lax.map(pair_outputs, (to_pairs(video_qkv), to_pairs(video_cross), to_pairs(audio_qkv), to_pairs(audio_cross), video_lens, audio_lens))
    video_out = combine(self_video, cross_video, gate_rows[0], gate_rows[1], clip_count)
    audio_out = combine(self_audio, cross_audio, gate_rows[2], gate_rows[3], clip_count)
    return (video_out, audio_out)
```

```python
import math

import jax
import jax.numpy as jnp
from jax import lax
from jax.experimental import pallas as pl
from jax.experimental.pallas import tpu as pltpu
from jax.sharding import PartitionSpec as P

MESH = pl.DeviceIdType.MESH
TILE = 8
Q_DEVICES = 4
AUDIO_BLOCKS = 3


def softmax_parts(scores, visible, scale):
    scores = jnp.where(visible, scores * scale, -1e30)
    row_max = jnp.max(scores, axis=1, keepdims=True)
    weights = jnp.exp(scores - row_max)
    return weights.astype(jnp.bfloat16), jnp.sum(weights, axis=1, keepdims=True)


def attend(queries, key_rows, values, visible, scale):
    scores = lax.dot_general(
        queries, key_rows, (((1,), (1,)), ((), ())), preferred_element_type=jnp.float32
    )
    weights, total = softmax_parts(scores, visible, scale)
    return jnp.dot(weights, values, preferred_element_type=jnp.float32) / total


def audio_tokens(count, rows):
    extra = rows - TILE
    column = lax.broadcasted_iota(jnp.int32, (1, count * rows), 1)
    rest = column - count * TILE
    device_first = lax.div(column, TILE)
    device_rest = lax.div(rest, extra)
    first = device_first * rows + (column - device_first * TILE)
    last = device_rest * rows + TILE + (rest - device_rest * extra)
    return jnp.where(rest >= 0, last, first)


def half_rows(tiles):
    return lax.broadcasted_iota(jnp.int32, tiles.shape, 1) < TILE // 2


def swap_halves(tiles):
    return jnp.concatenate([tiles[:, TILE // 2 :], tiles[:, : TILE // 2]], axis=1)


def exchange_and_attend(
    lens,
    gates,
    video_self,
    video_far,
    audio,
    video_out,
    audio_out,
    got_self,
    got_far,
    got_audio,
    audio_sets,
    made_video,
    made_audio,
    mixed_audio,
    sent,
    arrived,
    out_sent,
    out_arrived,
):
    me = lax.axis_index("seq")
    count = got_self.shape[1]
    chips = count // 2
    head_size = got_self.shape[3]
    video_rows = got_self.shape[2]
    audio_rows = got_audio.shape[1] // 6
    scale = 1.0 / math.sqrt(head_size)

    def partner(i):
        step = lax.div(i, 2)
        distance = chips // 2 - lax.div(step + 1, 2)
        offset = distance * (1 - 2 * lax.rem(step, 2)) + chips
        chip = lax.rem(lax.div(me, 2) + offset, chips)
        return chip * 2 + lax.rem(lax.rem(me, 2) + lax.rem(i, 2), 2)

    barrier = pltpu.get_barrier_semaphore()

    def greet(i, carry):
        pl.semaphore_signal(
            barrier, inc=1, device_id={"seq": lax.rem(me + i, count)}, device_id_type=MESH
        )
        return carry

    lax.fori_loop(1, count, greet, 0)
    pl.semaphore_wait(barrier, count - 1)

    key_values = pl.ds(1, 2)
    moves = (
        (video_self, lambda device: got_self.at[:, device]),
        (video_far.at[:, 0], lambda device: got_far.at[0, device]),
        (audio, lambda device: got_audio.at[device]),
        (video_far.at[:, key_values], lambda device: got_far.at[key_values, device]),
    )

    for j, (source, place) in enumerate(moves):
        pltpu.make_async_copy(source.at[me], place(me), arrived.at[j]).start()
    for j, (source, place) in enumerate(moves):

        def send(i, carry, j=j, source=source, place=place):
            other = partner(i)

            @pl.when(other != me)
            def _():
                pltpu.make_async_remote_copy(
                    src_ref=source.at[other],
                    dst_ref=place(me),
                    send_sem=sent.at[j],
                    recv_sem=arrived.at[j],
                    device_id={"seq": other},
                    device_id_type=MESH,
                ).start()

            return carry

        lax.fori_loop(0, count, send, 0)

    pltpu.make_async_copy(got_audio, got_audio, arrived.at[2]).wait()

    first_rows = count * TILE
    for j in range(6):
        whole = got_audio[:, pl.ds(TILE * j, TILE), :]
        audio_sets[j, pl.ds(0, first_rows)] = whole.reshape(first_rows, head_size)
        tiles = got_audio[:, pl.ds(TILE * (6 + j % 3), TILE), :].astype(jnp.float32)
        tiles = tiles.reshape(count // 2, 2, TILE, head_size)
        even, odd = tiles[:, 0], tiles[:, 1]
        if j < 3:
            odd = swap_halves(odd)
        else:
            even = swap_halves(even)
        joined = jnp.where(half_rows(even), even, odd).astype(jnp.bfloat16)
        audio_sets[j, pl.ds(first_rows, count * TILE // 2)] = joined.reshape(
            count * TILE // 2, head_size
        )

    video_visible = (
        lax.broadcasted_iota(jnp.int32, (1, count * video_rows), 1) < lens[0]
    )
    audio_visible = audio_tokens(count, audio_rows) < lens[1]

    def rows_of(ref):
        return ref[...].reshape(-1, head_size)

    pltpu.make_async_copy(got_self, got_self, arrived.at[0]).wait()

    def send_output(made, out, j, other):
        @pl.when(other != me)
        def _():
            pltpu.make_async_remote_copy(
                src_ref=made.at[other],
                dst_ref=out.at[me],
                send_sem=out_sent.at[j],
                recv_sem=out_arrived.at[j],
                device_id={"seq": other},
                device_id_type=MESH,
            ).start()

        @pl.when(other == me)
        def _():
            pltpu.make_async_copy(made.at[me], out.at[me], out_arrived.at[j]).start()

    def video_block(b, carry):
        first = lax.rem(lax.div(me, Q_DEVICES) + 1 + b, count // Q_DEVICES) * Q_DEVICES
        here = pl.ds(first, Q_DEVICES)
        own = attend(
            rows_of(got_self.at[0, here]),
            rows_of(got_self.at[1]),
            rows_of(got_self.at[2]),
            video_visible,
            scale,
        )
        far = attend(
            rows_of(video_cross_q.at[here]), audio_sets[4], audio_sets[5], audio_visible, scale
        )
        mixed = gates[0:1] * own + gates[1:2] * far
        made_video[here] = mixed.astype(jnp.bfloat16).reshape(Q_DEVICES, video_rows, head_size)

        def send(k, carry):
            send_output(made_video, video_out, 0, first + k)
            return carry

        lax.fori_loop(0, Q_DEVICES, send, 0)
        return carry

    video_cross_q = got_far.at[0]
    pltpu.make_async_copy(video_cross_q, video_cross_q, arrived.at[1]).wait()
    lax.fori_loop(0, count // Q_DEVICES, video_block, 0)

    video_cross_kv = got_far.at[key_values]
    pltpu.make_async_copy(video_cross_kv, video_cross_kv, arrived.at[3]).wait()
    block_rows = count * audio_rows // AUDIO_BLOCKS

    def audio_block(b, carry):
        here = pl.ds(pl.multiple_of(b * block_rows, TILE), block_rows)
        own = attend(audio_sets[0, here], audio_sets[1], audio_sets[2], audio_visible, scale)
        far = attend(
            audio_sets[3, here],
            rows_of(got_far.at[1]),
            rows_of(got_far.at[2]),
            video_visible,
            scale,
        )
        mixed_audio[here] = gates[2:3] * own + gates[3:4] * far
        return carry

    lax.fori_loop(0, AUDIO_BLOCKS, audio_block, 0)

    made_audio[:, pl.ds(0, TILE)] = (
        mixed_audio[pl.ds(0, first_rows)].astype(jnp.bfloat16).reshape(count, TILE, head_size)
    )
    rest = mixed_audio[pl.ds(first_rows, first_rows // 2)].reshape(count // 2, TILE, head_size)
    both = jnp.stack([rest, swap_halves(rest)], axis=1)
    made_audio[:, pl.ds(TILE, TILE)] = both.astype(jnp.bfloat16).reshape(count, TILE, head_size)

    def send_audio(i, carry):
        send_output(made_audio, audio_out, 1, partner(i))
        return carry

    lax.fori_loop(0, count, send_audio, 0)

    others = pl.ds(0, count - 1)
    for j, (source, _) in enumerate(moves):
        gone = source.at[others]
        pltpu.make_async_copy(gone, gone, sent.at[j]).wait()
    for j, (made, out) in enumerate(((made_video, video_out), (made_audio, audio_out))):
        pltpu.make_async_copy(made.at[others], made.at[others], out_sent.at[j]).wait()
        pltpu.make_async_copy(out, out, out_arrived.at[j]).wait()


def on_device(video_qkv, video_cross, audio_qkv, audio_cross, lengths, timestep, gate_table):
    count = lax.axis_size("seq")
    clip_count, head_count = video_qkv.shape[:2]
    video_rows, head_size = video_qkv.shape[3:]
    audio_rows = audio_qkv.shape[3]
    if clip_count * head_count != count or audio_rows != TILE * 3 // 2:
        raise ValueError("unexpected shapes")
    me = lax.axis_index("seq")
    clip, head = lax.div(me, head_count), lax.rem(me, head_count)

    lens = lax.dynamic_slice(lengths, (0, clip), (2, 1)).reshape(2)
    gates = lax.dynamic_slice(
        gate_table, (timestep[0], 0, head, 0), (1, gate_table.shape[1], 1, head_size)
    ).reshape(gate_table.shape[1], head_size)

    def pairs(tensor):
        return tensor.reshape((count,) + tensor.shape[2:])

    audio = jnp.concatenate([pairs(audio_qkv), pairs(audio_cross)], axis=1)
    tile_rows = audio[:, :, :TILE].reshape(count, 6 * TILE, head_size)
    rest = audio[:, :, TILE:].reshape(count, 2, 3, TILE // 2, head_size)
    rest = jnp.swapaxes(rest, 1, 2).reshape(count, 3 * TILE, head_size)
    audio = jnp.concatenate([tile_rows, rest], axis=1)

    bf16 = jnp.bfloat16
    video_out, audio_out = pl.pallas_call(
        exchange_and_attend,
        out_shape=(
            jax.ShapeDtypeStruct((count, video_rows, head_size), bf16),
            jax.ShapeDtypeStruct((count, 2 * TILE, head_size), bf16),
        ),
        in_specs=[
            pl.BlockSpec(memory_space=pltpu.SMEM),
            pl.BlockSpec(memory_space=pltpu.VMEM),
            pl.BlockSpec(memory_space=pl.ANY),
            pl.BlockSpec(memory_space=pl.ANY),
            pl.BlockSpec(memory_space=pl.ANY),
        ],
        out_specs=[pl.BlockSpec(memory_space=pl.ANY)] * 2,
        scratch_shapes=[
            pltpu.VMEM((3, count, video_rows, head_size), bf16),
            pltpu.VMEM((3, count, video_rows, head_size), bf16),
            pltpu.VMEM((count, 6 * audio_rows, head_size), bf16),
            pltpu.VMEM((6, count * audio_rows, head_size), bf16),
            pltpu.VMEM((count, video_rows, head_size), bf16),
            pltpu.VMEM((count, 2 * TILE, head_size), bf16),
            pltpu.VMEM((count * audio_rows, head_size), jnp.float32),
            pltpu.SemaphoreType.DMA((4,)),
            pltpu.SemaphoreType.DMA((4,)),
            pltpu.SemaphoreType.DMA((2,)),
            pltpu.SemaphoreType.DMA((2,)),
        ],
        compiler_params=pltpu.CompilerParams(
            collective_id=0, has_side_effects=True, vmem_limit_bytes=60 * 2**20
        ),
    )(lens, gates, pairs(video_qkv), pairs(video_cross), audio)
    return (
        video_out.reshape(clip_count, head_count, video_rows, head_size),
        audio_out[:, :audio_rows].reshape(clip_count, head_count, audio_rows, head_size),
    )


def solution(mesh):
    tokens = P("groups", None, None, "seq", None)
    made = P("groups", None, "seq", None)
    return jax.shard_map(
        on_device,
        mesh=mesh,
        in_specs=(tokens, tokens, tokens, tokens, P(None, "groups"), P("groups"), P()),
        out_specs=(made, made),
        check_vma=False,
    )
```

```python
import functools
import math

import jax
import jax.numpy as jnp
from jax import lax
from jax.experimental import pallas as pl
from jax.experimental.pallas import tpu as pltpu
from jax.sharding import PartitionSpec as P

MESH = pl.DeviceIdType.MESH
HALF_TILE = 4
Q_DEVICES = 4
AUDIO_BLOCKS = 3


def dot_rows(left, right):
    return lax.dot_general(
        left, right, (((1,), (1,)), ((), ())), preferred_element_type=jnp.float32
    )


def attend(queries, key_rows, values, visible, scale):
    scores = jnp.where(visible, dot_rows(queries, key_rows) * scale, -1e30)
    row_max = jnp.max(scores, axis=1, keepdims=True)
    weights = jnp.exp(scores - row_max)
    row_total = jnp.sum(weights, axis=1, keepdims=True)
    found = jnp.dot(weights.astype(jnp.bfloat16), values, preferred_element_type=jnp.float32)
    return found / row_total


def attend_part(queries, key_rows, values, visible, scale):
    scores = jnp.where(visible, dot_rows(key_rows, queries) * scale, -1e30)
    top = jnp.max(scores, axis=0, keepdims=True)
    weights = jnp.exp(scores - top)
    total = jnp.sum(weights, axis=0, keepdims=True)
    found = lax.dot_general(
        values,
        weights.astype(jnp.bfloat16),
        (((0,), (0,)), ((), ())),
        preferred_element_type=jnp.float32,
    )
    return found, top, total


def exchange_and_attend(
    head_count,
    lengths,
    timestep,
    gate_table,
    video_self,
    video_far,
    video_far_halves,
    audio_self_raw,
    audio_far_raw,
    video_out,
    audio_out,
    gates,
    raw,
    audio,
    got_self,
    got_query,
    got_kv,
    got_audio,
    got_audio_query,
    audio_sets,
    part_video,
    made_video,
    part_audio,
    half_found,
    half_stats,
    got_stats,
    made_audio,
    loaded,
    sent,
    arrived,
    stats_sent,
    stats_arrived,
    out_sent,
    out_arrived,
):
    me = lax.axis_index("seq")
    count = got_self.shape[1]
    half = count // 2
    chips = count // 2
    head_size = got_self.shape[3]
    video_rows = got_self.shape[2]
    audio_rows = raw.shape[3]
    audio_total = count * audio_rows
    scale = 1.0 / math.sqrt(head_size)
    my_chip, my_core = lax.div(me, 2), lax.rem(me, 2)
    mirror = lax.rem(me + half, count)
    my_half, my_place = lax.div(me, half), lax.rem(me, half)

    def at_offset(offset, core):
        return lax.rem(my_chip + offset + chips, chips) * 2 + core

    def partner(i):
        step = lax.div(i, 2)
        offset = (chips // 2 - lax.div(step + 1, 2)) * (1 - 2 * lax.rem(step, 2))
        return at_offset(offset, lax.rem(my_core + lax.rem(i, 2), 2))

    def near_target(i):
        step, core = lax.div(i, 2), lax.rem(i, 2)
        offset = (chips // 4 - lax.div(step + 1, 2)) * (1 - 2 * lax.rem(step, 2)) * (1 - 2 * core)
        slot = (chips // 4 - core - offset) * 2 + my_core
        return at_offset(offset, core), slot

    barrier = pltpu.get_barrier_semaphore()

    def greet(i, carry):
        pl.semaphore_signal(
            barrier, inc=1, device_id={"seq": lax.rem(me + i, count)}, device_id_type=MESH
        )
        return carry

    lax.fori_loop(1, count, greet, 0)

    loads = (
        pltpu.make_async_copy(audio_self_raw, raw.at[0], loaded.at[0]),
        pltpu.make_async_copy(audio_far_raw, raw.at[1], loaded.at[1]),
        pltpu.make_async_copy(gate_table, gates, loaded.at[2]),
    )
    for load in loads:
        load.start()
    for load in loads:
        load.wait()
    for side in range(2):
        for clip in range(raw.shape[1]):
            rows = raw[side, clip].astype(jnp.float32)
            rows = rows.reshape(3 * audio_rows, head_count, head_size)
            rows = jnp.swapaxes(rows, 0, 1).astype(jnp.bfloat16)
            audio[pl.ds(clip * head_count, head_count), pl.ds(3 * side, 3)] = rows.reshape(
                head_count, 3, audio_rows // HALF_TILE, HALF_TILE, head_size
            )

    pl.semaphore_wait(barrier, count - 1)

    keys_values = pl.ds(1, 2)

    def copy_to(source, place, j, other):
        return pltpu.make_async_remote_copy(
            src_ref=source,
            dst_ref=place,
            send_sem=sent.at[j],
            recv_sem=arrived.at[j],
            device_id={"seq": other},
            device_id_type=MESH,
        )

    def send_kv(i, carry):
        other, slot = near_target(i)
        source = video_far_halves.at[:, lax.rem(other, half), keys_values]
        place = got_kv.at[:, :, slot]

        @pl.when(other != me)
        def _():
            copy_to(source, place, 0, other).start()

        @pl.when(other == me)
        def _():
            pltpu.make_async_copy(source, place, arrived.at[0]).start()

        return carry

    lax.fori_loop(0, half, send_kv, 0)

    def mirror_of(device):
        return lax.rem(device + half, count)

    spread = {
        1: (lambda other: audio.at[other], got_audio.at[me]),
        2: (lambda other: audio.at[mirror_of(other), 3], got_audio_query.at[me]),
        3: (lambda other: video_self.at[other], got_self.at[:, me]),
        4: (lambda other: video_far.at[other, 0], got_query.at[me]),
    }

    def send_all(*kinds):
        for j in kinds:
            pltpu.make_async_copy(spread[j][0](me), spread[j][1], arrived.at[j]).start()

        for j in kinds:

            def send(i, carry, j=j):
                other = partner(i)

                @pl.when(other != me)
                def _():
                    copy_to(spread[j][0](other), spread[j][1], j, other).start()

                return carry

            lax.fori_loop(0, count, send, 0)

    send_all(1)
    send_all(2)
    send_all(3)

    def wait_whole(ref, sem):
        pltpu.make_async_copy(ref, ref, sem).wait()

    step_gates = timestep[0]

    def gate(row, device):
        head = lax.rem(device, head_count)
        return gates[pl.ds(step_gates, 1), row, pl.ds(head, 1), :].reshape(1, head_size)

    wait_whole(got_audio, arrived.at[1])
    wait_whole(got_audio_query, arrived.at[2])
    for j in range(6):
        audio_sets[j] = got_audio[:, j].reshape(audio_total, head_size)
    audio_sets[6] = got_audio_query[...].reshape(audio_total, head_size)
    wait_whole(got_kv, arrived.at[0])

    block = audio_total // AUDIO_BLOCKS
    first_near = lax.rem(my_chip - chips // 4 + my_core + chips, chips) * 2 * video_rows
    position = first_near + lax.broadcasted_iota(jnp.int32, (half * video_rows, block), 0)
    position = jnp.where(
        position >= count * video_rows, position - count * video_rows, position
    )

    def rows_of(ref):
        return ref[...].reshape(-1, head_size)

    def cross_part(i, carry):
        kind, b = lax.div(i, AUDIO_BLOCKS), lax.rem(i, AUDIO_BLOCKS)
        pair = lax.rem(me + kind * half, count)
        side = lax.div(pair, half)
        found, top, total = attend_part(
            audio_sets[3 + 3 * kind, pl.ds(pl.multiple_of(b * block, block), block)],
            rows_of(got_kv.at[side, 0]),
            rows_of(got_kv.at[side, 1]),
            position < lengths[0, lax.div(pair, head_count)],
            scale,
        )
        half_found[i] = found
        half_stats[i] = jnp.concatenate([top, total], axis=0)
        return carry

    lax.fori_loop(0, 2 * AUDIO_BLOCKS, cross_part, 0)
    stats_copy = pltpu.make_async_remote_copy(
        src_ref=half_stats,
        dst_ref=got_stats,
        send_sem=stats_sent,
        recv_sem=stats_arrived,
        device_id={"seq": mirror},
        device_id_type=MESH,
    )
    stats_copy.start()
    send_all(4)

    my_clip = lax.div(me, head_count)
    audio_visible = (
        lax.broadcasted_iota(jnp.int32, (1, audio_total), 1) < lengths[1, my_clip]
    )
    video_visible = (
        lax.broadcasted_iota(jnp.int32, (1, count * video_rows), 1) < lengths[0, my_clip]
    )

    def audio_block(b, carry):
        here = pl.ds(pl.multiple_of(b * block, block), block)
        own = attend(audio_sets[0, here], audio_sets[1], audio_sets[2], audio_visible, scale)
        part_audio[0, here] = gate(2, me) * own
        part_audio[1, here] = jnp.zeros_like(own)
        return carry

    lax.fori_loop(0, AUDIO_BLOCKS, audio_block, 0)

    stats_copy.wait()

    def join_parts(i, carry):
        kind, b = lax.div(i, AUDIO_BLOCKS), lax.rem(i, AUDIO_BLOCKS)
        pair = lax.rem(me + kind * half, count)
        mine = half_stats[i]
        theirs = got_stats[(1 - kind) * AUDIO_BLOCKS + b]
        top = jnp.maximum(mine[0:1], theirs[0:1])
        weight = jnp.exp(mine[0:1] - top)
        total = mine[1:2] * weight + theirs[1:2] * jnp.exp(theirs[0:1] - top)
        found = half_found[i] * (weight / total)
        here = pl.ds(pl.multiple_of(b * block, block), block)
        part_audio[kind, here] = part_audio[kind, here] + gate(3, pair) * found.T
        return carry

    lax.fori_loop(0, 2 * AUDIO_BLOCKS, join_parts, 0)
    for kind in range(2):
        side = lax.rem(my_half + kind, 2)
        made_audio[side] = (
            part_audio[kind]
            .astype(jnp.bfloat16)
            .reshape(count, audio_rows // HALF_TILE, HALF_TILE, head_size)
        )

    def send_output(made, place, j, other):
        @pl.when(other != me)
        def _():
            pltpu.make_async_remote_copy(
                src_ref=made,
                dst_ref=place,
                send_sem=out_sent.at[j],
                recv_sem=out_arrived.at[j],
                device_id={"seq": other},
                device_id_type=MESH,
            ).start()

        @pl.when(other == me)
        def _():
            pltpu.make_async_copy(made, place, out_arrived.at[j]).start()

    def video_self_block(b, carry):
        here = pl.ds(b * Q_DEVICES, Q_DEVICES)
        own = attend(
            rows_of(got_self.at[0, here]),
            rows_of(got_self.at[1]),
            rows_of(got_self.at[2]),
            video_visible,
            scale,
        )
        part_video[here] = (gate(0, me) * own).reshape(Q_DEVICES, video_rows, head_size)
        return carry

    def send_audio(i, carry):
        other = partner(i)
        send_output(made_audio.at[:, other], audio_out.at[my_half, :, my_place], 1, other)
        return carry

    lax.fori_loop(0, count, send_audio, 0)

    wait_whole(got_self, arrived.at[3])
    lax.fori_loop(0, count // Q_DEVICES, video_self_block, 0)

    wait_whole(got_query, arrived.at[4])

    def video_cross_block(b, carry):
        first = lax.rem(lax.div(me, Q_DEVICES) + 1 + b, count // Q_DEVICES) * Q_DEVICES
        here = pl.ds(first, Q_DEVICES)
        far = attend(
            rows_of(got_query.at[here]), audio_sets[4], audio_sets[5], audio_visible, scale
        )
        mixed = part_video[here] + (gate(1, me) * far).reshape(Q_DEVICES, video_rows, head_size)
        made_video[here] = mixed.astype(jnp.bfloat16)

        def send(k, carry):
            other = first + k
            send_output(made_video.at[other], video_out.at[me], 0, other)
            return carry

        lax.fori_loop(0, Q_DEVICES, send, 0)
        return carry

    lax.fori_loop(0, count // Q_DEVICES, video_cross_block, 0)

    others = pl.ds(0, count - 1)
    wait_whole(video_far_halves.at[:, pl.ds(0, half - 1), keys_values], sent.at[0])
    wait_whole(audio.at[others], sent.at[1])
    wait_whole(audio.at[others, 3], sent.at[2])
    wait_whole(video_self.at[others], sent.at[3])
    wait_whole(video_far.at[others, 0], sent.at[4])
    wait_whole(made_video.at[others], out_sent.at[0])
    wait_whole(made_audio.at[:, others], out_sent.at[1])
    wait_whole(video_out, out_arrived.at[0])
    wait_whole(audio_out, out_arrived.at[1])


def on_device(video_qkv, video_cross, audio_qkv, audio_cross, lengths, timestep, gate_table):
    count = lax.axis_size("seq")
    half = count // 2
    clip_count, head_count = video_qkv.shape[:2]
    video_rows, head_size = video_qkv.shape[3:]
    audio_rows = audio_qkv.shape[3]
    if clip_count * head_count != count or audio_rows % HALF_TILE:
        raise ValueError("unexpected shapes")
    quarters = audio_rows // HALF_TILE
    audio_total = count * audio_rows
    block = audio_total // AUDIO_BLOCKS

    video_self = video_qkv.reshape(count, 3, video_rows, head_size)
    video_far = video_cross.reshape(count, 3, video_rows, head_size)
    video_far_halves = video_cross.reshape(2, half, 3, video_rows, head_size)

    def heads_inside(tensor):
        return jnp.transpose(tensor, (0, 2, 3, 1, 4))

    bf16, f32 = jnp.bfloat16, jnp.float32
    anywhere = pl.BlockSpec(memory_space=pl.ANY)
    scalars = pl.BlockSpec(memory_space=pltpu.SMEM)
    video_out, audio_out = pl.pallas_call(
        functools.partial(exchange_and_attend, head_count),
        out_shape=(
            jax.ShapeDtypeStruct((count, video_rows, head_size), bf16),
            jax.ShapeDtypeStruct((2, 2, half, quarters, HALF_TILE, head_size), bf16),
        ),
        in_specs=[scalars, scalars] + [anywhere] * 6,
        out_specs=[anywhere] * 2,
        scratch_shapes=[
            pltpu.VMEM(gate_table.shape, f32),
            pltpu.VMEM((2, clip_count, 3, audio_rows, head_count, head_size), bf16),
            pltpu.VMEM((count, 6, quarters, HALF_TILE, head_size), bf16),
            pltpu.VMEM((3, count, video_rows, head_size), bf16),
            pltpu.VMEM((count, video_rows, head_size), bf16),
            pltpu.VMEM((2, 2, half, video_rows, head_size), bf16),
            pltpu.VMEM((count, 6, quarters, HALF_TILE, head_size), bf16),
            pltpu.VMEM((count, quarters, HALF_TILE, head_size), bf16),
            pltpu.VMEM((7, audio_total, head_size), bf16),
            pltpu.VMEM((count, video_rows, head_size), f32),
            pltpu.VMEM((count, video_rows, head_size), bf16),
            pltpu.VMEM((2, audio_total, head_size), f32),
            pltpu.VMEM((2 * AUDIO_BLOCKS, head_size, block), f32),
            pltpu.VMEM((2 * AUDIO_BLOCKS, 2, block), f32),
            pltpu.VMEM((2 * AUDIO_BLOCKS, 2, block), f32),
            pltpu.VMEM((2, count, quarters, HALF_TILE, head_size), bf16),
            pltpu.SemaphoreType.DMA((3,)),
            pltpu.SemaphoreType.DMA((5,)),
            pltpu.SemaphoreType.DMA((5,)),
            pltpu.SemaphoreType.DMA,
            pltpu.SemaphoreType.DMA,
            pltpu.SemaphoreType.DMA((2,)),
            pltpu.SemaphoreType.DMA((2,)),
        ],
        compiler_params=pltpu.CompilerParams(
            collective_id=0, has_side_effects=True, vmem_limit_bytes=62 * 2**20
        ),
    )(
        lengths,
        timestep,
        gate_table,
        video_self,
        video_far,
        video_far_halves,
        heads_inside(audio_qkv),
        heads_inside(audio_cross),
    )
    audio_sum = audio_out[0].astype(f32) + audio_out[1].astype(f32)
    return (
        video_out.reshape(clip_count, head_count, video_rows, head_size),
        audio_sum.astype(bf16).reshape(clip_count, head_count, audio_rows, head_size),
    )


def solution(mesh):
    tokens = P("groups", None, None, "seq", None)
    made = P("groups", None, "seq", None)
    return jax.shard_map(
        on_device,
        mesh=mesh,
        in_specs=(tokens, tokens, tokens, tokens, P(None, "groups"), P("groups"), P()),
        out_specs=(made, made),
        check_vma=False,
    )
```

```python
import functools
import math

import jax
import jax.numpy as jnp
from jax import lax
from jax.experimental import pallas as pl
from jax.experimental.pallas import tpu as pltpu
from jax.sharding import PartitionSpec as P

MESH = pl.DeviceIdType.MESH
HALF_TILE = 4
Q_DEVICES = 4
AUDIO_BLOCKS = 3


def dot_rows(left, right):
    return lax.dot_general(
        left, right, (((1,), (1,)), ((), ())), preferred_element_type=jnp.float32
    )


def attend(queries, key_rows, values, visible, scale):
    scores = jnp.where(visible, dot_rows(queries, key_rows) * scale, -1e30)
    row_max = jnp.max(scores, axis=1, keepdims=True)
    weights = jnp.exp(scores - row_max)
    row_total = jnp.sum(weights, axis=1, keepdims=True)
    found = jnp.dot(weights.astype(jnp.bfloat16), values, preferred_element_type=jnp.float32)
    return found / row_total


def attend_part(queries, key_rows, values, visible, scale):
    scores = jnp.where(visible, dot_rows(key_rows, queries) * scale, -1e30)
    top = jnp.max(scores, axis=0, keepdims=True)
    weights = jnp.exp(scores - top)
    total = jnp.sum(weights, axis=0, keepdims=True)
    found = lax.dot_general(
        values,
        weights.astype(jnp.bfloat16),
        (((0,), (0,)), ((), ())),
        preferred_element_type=jnp.float32,
    )
    return found, top, total


def exchange_and_attend(
    head_count,
    lengths,
    timestep,
    gate_table,
    video_self,
    video_far,
    video_far_halves,
    audio_self_raw,
    audio_far_raw,
    video_out,
    audio_out,
    gates,
    raw,
    audio,
    got_self,
    got_query,
    got_kv,
    got_audio,
    got_audio_query,
    audio_sets,
    part_video,
    made_video,
    part_audio,
    half_found,
    half_stats,
    got_stats,
    made_audio,
    got_made_audio,
    final_audio,
    known_quarter,
    known_half,
    loaded,
    sent,
    arrived,
    stats_sent,
    stats_arrived,
    out_sent,
    out_arrived,
):
    me = lax.axis_index("seq")
    count = got_self.shape[1]
    half = count // 2
    chips = count // 2
    head_size = got_self.shape[3]
    video_rows = got_self.shape[2]
    audio_rows = raw.shape[3]
    audio_total = count * audio_rows
    scale = 1.0 / math.sqrt(head_size)
    my_chip, my_core = lax.div(me, 2), lax.rem(me, 2)
    mirror = lax.rem(me + half, count)
    my_half, my_place = lax.div(me, half), lax.rem(me, half)

    def at_offset(offset, core):
        return lax.rem(my_chip + offset + chips, chips) * 2 + core

    def partner(i):
        step = lax.div(i, 2)
        offset = (chips // 2 - lax.div(step + 1, 2)) * (1 - 2 * lax.rem(step, 2))
        return at_offset(offset, lax.rem(my_core + lax.rem(i, 2), 2))

    def near_target(i):
        step, core = lax.div(i, 2), lax.rem(i, 2)
        offset = (chips // 4 - lax.div(step + 1, 2)) * (1 - 2 * lax.rem(step, 2)) * (1 - 2 * core)
        slot = (chips // 4 - core - offset) * 2 + my_core
        return at_offset(offset, core), slot

    loads = (
        pltpu.make_async_copy(audio_self_raw, raw.at[0], loaded.at[0]),
        pltpu.make_async_copy(audio_far_raw, raw.at[1], loaded.at[1]),
        pltpu.make_async_copy(gate_table, gates, loaded.at[2]),
    )
    for load in loads:
        load.start()

    reach = chips // 8
    barrier = pltpu.get_barrier_semaphore()

    def greet(i, carry):
        other = at_offset(lax.div(i, 2) - reach, lax.rem(i, 2))

        @pl.when(other != me)
        def _():
            pl.semaphore_signal(barrier, inc=1, device_id={"seq": other}, device_id_type=MESH)

        return carry

    lax.fori_loop(0, 4 * reach + 2, greet, 0)
    pl.semaphore_wait(barrier, 4 * reach + 1)

    def pass_on(known, distance):
        for offset in (-distance, distance):
            pl.semaphore_signal(
                known,
                inc=1,
                device_id={"seq": at_offset(offset, my_core)},
                device_id_type=MESH,
            )

    pass_on(known_quarter, reach)

    keys_values = pl.ds(1, 2)

    def copy_to(source, place, j, other):
        return pltpu.make_async_remote_copy(
            src_ref=source,
            dst_ref=place,
            send_sem=sent.at[j],
            recv_sem=arrived.at[j],
            device_id={"seq": other},
            device_id_type=MESH,
        )

    def send_kv(i, carry):
        other, slot = near_target(i)
        source = video_far_halves.at[:, lax.rem(other, half), keys_values]
        place = got_kv.at[:, :, slot]

        @pl.when(other != me)
        def _():
            copy_to(source, place, 0, other).start()

        @pl.when(other == me)
        def _():
            pltpu.make_async_copy(source, place, arrived.at[0]).start()

        return carry

    first_close = 4 * (chips // 4 - reach) - 2
    lax.fori_loop(first_close, half, send_kv, 0)

    for load in loads:
        load.wait()
    for side in range(2):
        for clip in range(raw.shape[1]):
            rows = raw[side, clip].astype(jnp.float32)
            rows = rows.reshape(3 * audio_rows, head_count, head_size)
            rows = jnp.swapaxes(rows, 0, 1).astype(jnp.bfloat16)
            audio[pl.ds(clip * head_count, head_count), pl.ds(3 * side, 3)] = rows.reshape(
                head_count, 3, audio_rows // HALF_TILE, HALF_TILE, head_size
            )

    pl.semaphore_wait(known_quarter, 2)
    pass_on(known_half, 2 * reach)
    lax.fori_loop(0, first_close, send_kv, 0)
    pl.semaphore_wait(known_half, 2)

    def mirror_of(device):
        return lax.rem(device + half, count)

    spread = {
        1: (lambda other: audio.at[other], got_audio.at[me]),
        2: (lambda other: audio.at[mirror_of(other), 3], got_audio_query.at[me]),
        3: (lambda other: video_self.at[other], got_self.at[:, me]),
        4: (lambda other: video_far.at[other, 0], got_query.at[me]),
    }

    def send_all(*kinds):
        for j in kinds:
            pltpu.make_async_copy(spread[j][0](me), spread[j][1], arrived.at[j]).start()

        for j in kinds:

            def send(i, carry, j=j):
                other = partner(i)

                @pl.when(other != me)
                def _():
                    copy_to(spread[j][0](other), spread[j][1], j, other).start()

                return carry

            lax.fori_loop(0, count, send, 0)

    send_all(1)
    send_all(2)
    send_all(3)

    def wait_whole(ref, sem):
        pltpu.make_async_copy(ref, ref, sem).wait()

    step_gates = timestep[0]

    def gate(row, device):
        head = lax.rem(device, head_count)
        return gates[pl.ds(step_gates, 1), row, pl.ds(head, 1), :].reshape(1, head_size)

    wait_whole(got_audio, arrived.at[1])
    wait_whole(got_audio_query, arrived.at[2])
    for j in range(6):
        audio_sets[j] = got_audio[:, j].reshape(audio_total, head_size)
    audio_sets[6] = got_audio_query[...].reshape(audio_total, head_size)
    wait_whole(got_kv, arrived.at[0])

    block = audio_total // AUDIO_BLOCKS
    first_near = lax.rem(my_chip - chips // 4 + my_core + chips, chips) * 2 * video_rows
    position = first_near + lax.broadcasted_iota(jnp.int32, (half * video_rows, block), 0)
    position = jnp.where(
        position >= count * video_rows, position - count * video_rows, position
    )

    def rows_of(ref):
        return ref[...].reshape(-1, head_size)

    def cross_part(i, carry):
        kind, b = lax.div(i, AUDIO_BLOCKS), lax.rem(i, AUDIO_BLOCKS)
        pair = lax.rem(me + kind * half, count)
        side = lax.div(pair, half)
        found, top, total = attend_part(
            audio_sets[3 + 3 * kind, pl.ds(pl.multiple_of(b * block, block), block)],
            rows_of(got_kv.at[side, 0]),
            rows_of(got_kv.at[side, 1]),
            position < lengths[0, lax.div(pair, head_count)],
            scale,
        )
        half_found[i] = found
        half_stats[i] = jnp.concatenate([top, total], axis=0)
        return carry

    lax.fori_loop(0, 2 * AUDIO_BLOCKS, cross_part, 0)
    stats_copy = pltpu.make_async_remote_copy(
        src_ref=half_stats,
        dst_ref=got_stats,
        send_sem=stats_sent,
        recv_sem=stats_arrived,
        device_id={"seq": mirror},
        device_id_type=MESH,
    )
    stats_copy.start()
    send_all(4)

    my_clip = lax.div(me, head_count)
    audio_visible = (
        lax.broadcasted_iota(jnp.int32, (1, audio_total), 1) < lengths[1, my_clip]
    )
    video_visible = (
        lax.broadcasted_iota(jnp.int32, (1, count * video_rows), 1) < lengths[0, my_clip]
    )

    def audio_block(b, carry):
        here = pl.ds(pl.multiple_of(b * block, block), block)
        own = attend(audio_sets[0, here], audio_sets[1], audio_sets[2], audio_visible, scale)
        part_audio[0, here] = gate(2, me) * own
        part_audio[1, here] = jnp.zeros_like(own)
        return carry

    lax.fori_loop(0, AUDIO_BLOCKS, audio_block, 0)

    stats_copy.wait()

    def join_parts(i, carry):
        kind, b = lax.div(i, AUDIO_BLOCKS), lax.rem(i, AUDIO_BLOCKS)
        pair = lax.rem(me + kind * half, count)
        mine = half_stats[i]
        theirs = got_stats[(1 - kind) * AUDIO_BLOCKS + b]
        top = jnp.maximum(mine[0:1], theirs[0:1])
        weight = jnp.exp(mine[0:1] - top)
        total = mine[1:2] * weight + theirs[1:2] * jnp.exp(theirs[0:1] - top)
        found = half_found[i] * (weight / total)
        here = pl.ds(pl.multiple_of(b * block, block), block)
        part_audio[kind, here] = part_audio[kind, here] + gate(3, pair) * found.T
        return carry

    lax.fori_loop(0, 2 * AUDIO_BLOCKS, join_parts, 0)
    for kind in range(2):
        side = lax.rem(my_half + kind, 2)
        made_audio[side] = (
            part_audio[kind]
            .astype(jnp.bfloat16)
            .reshape(count, audio_rows // HALF_TILE, HALF_TILE, head_size)
        )

    def send_output(made, place, j, other):
        @pl.when(other != me)
        def _():
            pltpu.make_async_remote_copy(
                src_ref=made,
                dst_ref=place,
                send_sem=out_sent.at[j],
                recv_sem=out_arrived.at[j],
                device_id={"seq": other},
                device_id_type=MESH,
            ).start()

        @pl.when(other == me)
        def _():
            pltpu.make_async_copy(made, place, out_arrived.at[j]).start()

    def video_self_block(b, carry):
        here = pl.ds(b * Q_DEVICES, Q_DEVICES)
        own = attend(
            rows_of(got_self.at[0, here]),
            rows_of(got_self.at[1]),
            rows_of(got_self.at[2]),
            video_visible,
            scale,
        )
        part_video[here] = (gate(0, me) * own).reshape(Q_DEVICES, video_rows, head_size)
        return carry

    def send_audio(i, carry):
        other = partner(i)
        send_output(made_audio.at[:, other], got_made_audio.at[my_half, :, my_place], 1, other)
        return carry

    lax.fori_loop(0, count, send_audio, 0)

    wait_whole(got_self, arrived.at[3])
    lax.fori_loop(0, count // Q_DEVICES, video_self_block, 0)

    wait_whole(got_query, arrived.at[4])

    def video_cross_block(b, carry):
        blocks = count // Q_DEVICES
        offset = (blocks // 2 - lax.div(b + 1, 2)) * (1 - 2 * lax.rem(b, 2))
        first = lax.rem(lax.div(me, Q_DEVICES) + offset + blocks, blocks) * Q_DEVICES
        here = pl.ds(first, Q_DEVICES)
        far = attend(
            rows_of(got_query.at[here]), audio_sets[4], audio_sets[5], audio_visible, scale
        )
        mixed = part_video[here] + (gate(1, me) * far).reshape(Q_DEVICES, video_rows, head_size)
        made_video[here] = mixed.astype(jnp.bfloat16)

        def send(k, carry):
            other = first + k
            send_output(made_video.at[other], video_out.at[me], 0, other)
            return carry

        lax.fori_loop(0, Q_DEVICES, send, 0)
        return carry

    lax.fori_loop(0, count // Q_DEVICES, video_cross_block, 0)

    wait_whole(got_made_audio, out_arrived.at[1])
    whole_audio = got_made_audio[0].astype(jnp.float32) + got_made_audio[1].astype(jnp.float32)
    whole_audio = whole_audio.reshape(count // head_count, head_count, audio_rows, head_size)
    for clip in range(count // head_count):
        final_audio[clip] = jnp.swapaxes(whole_audio[clip], 0, 1).astype(jnp.bfloat16)
    keep_audio = pltpu.make_async_copy(final_audio, audio_out, loaded.at[0])
    keep_audio.start()
    keep_audio.wait()

    others = pl.ds(0, count - 1)
    wait_whole(video_far_halves.at[:, pl.ds(0, half - 1), keys_values], sent.at[0])
    wait_whole(audio.at[others], sent.at[1])
    wait_whole(audio.at[others, 3], sent.at[2])
    wait_whole(video_self.at[others], sent.at[3])
    wait_whole(video_far.at[others, 0], sent.at[4])
    wait_whole(made_video.at[others], out_sent.at[0])
    wait_whole(made_audio.at[:, others], out_sent.at[1])
    wait_whole(video_out, out_arrived.at[0])


def on_device(video_qkv, video_cross, audio_qkv, audio_cross, lengths, timestep, gate_table):
    count = lax.axis_size("seq")
    half = count // 2
    clip_count, head_count = video_qkv.shape[:2]
    video_rows, head_size = video_qkv.shape[3:]
    audio_rows = audio_qkv.shape[3]
    if clip_count * head_count != count or audio_rows % HALF_TILE:
        raise ValueError("unexpected shapes")
    quarters = audio_rows // HALF_TILE
    audio_total = count * audio_rows
    block = audio_total // AUDIO_BLOCKS

    video_self = video_qkv.reshape(count, 3, video_rows, head_size)
    video_far = video_cross.reshape(count, 3, video_rows, head_size)
    video_far_halves = video_cross.reshape(2, half, 3, video_rows, head_size)

    def heads_inside(tensor):
        return jnp.transpose(tensor, (0, 2, 3, 1, 4))

    bf16, f32 = jnp.bfloat16, jnp.float32
    anywhere = pl.BlockSpec(memory_space=pl.ANY)
    scalars = pl.BlockSpec(memory_space=pltpu.SMEM)
    video_out, audio_out = pl.pallas_call(
        functools.partial(exchange_and_attend, head_count),
        out_shape=(
            jax.ShapeDtypeStruct((count, video_rows, head_size), bf16),
            jax.ShapeDtypeStruct((clip_count, audio_rows, head_count, head_size), bf16),
        ),
        in_specs=[scalars, scalars] + [anywhere] * 6,
        out_specs=[anywhere] * 2,
        scratch_shapes=[
            pltpu.VMEM(gate_table.shape, f32),
            pltpu.VMEM((2, clip_count, 3, audio_rows, head_count, head_size), bf16),
            pltpu.VMEM((count, 6, quarters, HALF_TILE, head_size), bf16),
            pltpu.VMEM((3, count, video_rows, head_size), bf16),
            pltpu.VMEM((count, video_rows, head_size), bf16),
            pltpu.VMEM((2, 2, half, video_rows, head_size), bf16),
            pltpu.VMEM((count, 6, quarters, HALF_TILE, head_size), bf16),
            pltpu.VMEM((count, quarters, HALF_TILE, head_size), bf16),
            pltpu.VMEM((7, audio_total, head_size), bf16),
            pltpu.VMEM((count, video_rows, head_size), f32),
            pltpu.VMEM((count, video_rows, head_size), bf16),
            pltpu.VMEM((2, audio_total, head_size), f32),
            pltpu.VMEM((2 * AUDIO_BLOCKS, head_size, block), f32),
            pltpu.VMEM((2 * AUDIO_BLOCKS, 2, block), f32),
            pltpu.VMEM((2 * AUDIO_BLOCKS, 2, block), f32),
            pltpu.VMEM((2, count, quarters, HALF_TILE, head_size), bf16),
            pltpu.VMEM((2, 2, half, quarters, HALF_TILE, head_size), bf16),
            pltpu.VMEM((clip_count, audio_rows, head_count, head_size), bf16),
            pltpu.SemaphoreType.REGULAR,
            pltpu.SemaphoreType.REGULAR,
            pltpu.SemaphoreType.DMA((3,)),
            pltpu.SemaphoreType.DMA((5,)),
            pltpu.SemaphoreType.DMA((5,)),
            pltpu.SemaphoreType.DMA,
            pltpu.SemaphoreType.DMA,
            pltpu.SemaphoreType.DMA((2,)),
            pltpu.SemaphoreType.DMA((2,)),
        ],
        compiler_params=pltpu.CompilerParams(
            collective_id=0, has_side_effects=True, vmem_limit_bytes=62 * 2**20
        ),
    )(
        lengths,
        timestep,
        gate_table,
        video_self,
        video_far,
        video_far_halves,
        heads_inside(audio_qkv),
        heads_inside(audio_cross),
    )
    return (
        video_out.reshape(clip_count, head_count, video_rows, head_size),
        jnp.swapaxes(audio_out, 1, 2),
    )


def solution(mesh):
    tokens = P("groups", None, None, "seq", None)
    made = P("groups", None, "seq", None)
    return jax.shard_map(
        on_device,
        mesh=mesh,
        in_specs=(tokens, tokens, tokens, tokens, P(None, "groups"), P("groups"), P()),
        out_specs=(made, made),
        check_vma=False,
    )
```

```python
import functools
import math

import jax
import jax.numpy as jnp
from jax import lax
from jax.experimental import pallas as pl
from jax.experimental.pallas import tpu as pltpu
from jax.sharding import PartitionSpec as P

MESH = pl.DeviceIdType.MESH
HALF_TILE = 4
Q_DEVICES = 4
AUDIO_BLOCKS = 3


def dot_rows(left, right):
    return lax.dot_general(
        left, right, (((1,), (1,)), ((), ())), preferred_element_type=jnp.float32
    )


def attend(queries, key_rows, values, visible, scale):
    scores = jnp.where(visible, dot_rows(queries, key_rows) * scale, -1e30)
    row_max = jnp.max(scores, axis=1, keepdims=True)
    weights = jnp.exp(scores - row_max)
    row_total = jnp.sum(weights, axis=1, keepdims=True)
    found = jnp.dot(weights.astype(jnp.bfloat16), values, preferred_element_type=jnp.float32)
    return found / row_total


def attend_part(queries, key_rows, values, visible, scale):
    scores = jnp.where(visible, dot_rows(key_rows, queries) * scale, -1e30)
    top = jnp.max(scores, axis=0, keepdims=True)
    weights = jnp.exp(scores - top)
    total = jnp.sum(weights, axis=0, keepdims=True)
    found = lax.dot_general(
        values,
        weights.astype(jnp.bfloat16),
        (((0,), (0,)), ((), ())),
        preferred_element_type=jnp.float32,
    )
    return found / total, top + jnp.log(total)


def exchange_and_attend(
    head_count,
    timestep,
    lengths_given,
    gate_table,
    video_self,
    video_far,
    video_far_halves,
    audio_self_raw,
    audio_far_raw,
    video_out,
    audio_out,
    lengths,
    gates,
    raw,
    audio,
    got_self,
    got_query,
    got_kv,
    got_audio,
    got_audio_query,
    audio_sets,
    part_video,
    made_video,
    part_audio,
    half_found,
    half_stats,
    got_stats,
    made_audio,
    got_made_audio,
    final_audio,
    known,
    loaded,
    sent,
    arrived,
    stats_sent,
    stats_arrived,
    out_sent,
    out_arrived,
):
    me = lax.axis_index("seq")
    count = got_self.shape[1]
    half = count // 2
    chips = count // 2
    head_size = got_self.shape[3]
    video_rows = got_self.shape[2]
    audio_rows = raw.shape[3]
    audio_total = count * audio_rows
    scale = 1.0 / math.sqrt(head_size)
    my_chip, my_core = lax.div(me, 2), lax.rem(me, 2)
    mirror = lax.rem(me + half, count)
    my_half, my_place = lax.div(me, half), lax.rem(me, half)

    def at_offset(offset, core):
        return lax.rem(my_chip + offset + chips, chips) * 2 + core

    def partner(i):
        step = lax.div(i, 2)
        offset = (chips // 2 - lax.div(step + 1, 2)) * (1 - 2 * lax.rem(step, 2))
        return at_offset(offset, lax.rem(my_core + lax.rem(i, 2), 2))

    def near_target(i):
        step, core = lax.div(i, 2), lax.rem(i, 2)
        offset = (chips // 4 - lax.div(step + 1, 2)) * (1 - 2 * lax.rem(step, 2)) * (1 - 2 * core)
        slot = (chips // 4 - core - offset) * 2 + my_core
        return at_offset(offset, core), slot

    loads = (
        pltpu.make_async_copy(audio_self_raw, raw.at[0], loaded.at[0]),
        pltpu.make_async_copy(audio_far_raw, raw.at[1], loaded.at[1]),
        pltpu.make_async_copy(gate_table, gates, loaded.at[2]),
        pltpu.make_async_copy(lengths_given, lengths, loaded.at[3]),
    )
    for load in loads:
        load.start()

    barrier = pltpu.get_barrier_semaphore()

    def greet(i, carry):
        other = at_offset(lax.div(i, 2) - 1, lax.rem(i, 2))

        @pl.when(other != me)
        def _():
            pl.semaphore_signal(barrier, inc=1, device_id={"seq": other}, device_id_type=MESH)

        return carry

    lax.fori_loop(0, 6, greet, 0)
    pl.semaphore_wait(barrier, 5)

    def pass_on(step, distance):
        for offset in (-distance, distance):
            pl.semaphore_signal(
                known.at[step],
                inc=1,
                device_id={"seq": at_offset(offset, my_core)},
                device_id_type=MESH,
            )

    keys_values = pl.ds(1, 2)

    def copy_to(source, place, j, other):
        return pltpu.make_async_remote_copy(
            src_ref=source,
            dst_ref=place,
            send_sem=sent.at[j],
            recv_sem=arrived.at[j],
            device_id={"seq": other},
            device_id_type=MESH,
        )

    def send_kv(i, carry):
        other, slot = near_target(i)
        source = video_far_halves.at[:, lax.rem(other, half), keys_values]
        place = got_kv.at[:, :, slot]

        @pl.when(other != me)
        def _():
            copy_to(source, place, 0, other).start()

        @pl.when(other == me)
        def _():
            pltpu.make_async_copy(source, place, arrived.at[0]).start()

        return carry

    quarter = chips // 4
    reach, unsent = 1, half
    for step in range(known.shape[0]):
        pass_on(step, reach)
        start = max(0, 4 * (quarter - reach) - 2)
        lax.fori_loop(start, unsent, send_kv, 0)
        unsent, reach = start, 2 * reach
        if step < known.shape[0] - 1:
            pl.semaphore_wait(known.at[step], 2)

    for load in loads:
        load.wait()
    for side in range(2):
        for clip in range(raw.shape[1]):
            rows = raw[side, clip].astype(jnp.float32)
            rows = rows.reshape(3 * audio_rows, head_count, head_size)
            rows = jnp.swapaxes(rows, 0, 1).astype(jnp.bfloat16)
            audio[pl.ds(clip * head_count, head_count), pl.ds(3 * side, 3)] = rows.reshape(
                head_count, 3, audio_rows // HALF_TILE, HALF_TILE, head_size
            )

    pl.semaphore_wait(known.at[known.shape[0] - 1], 2)

    def mirror_of(device):
        return lax.rem(device + half, count)

    spread = {
        1: (lambda other: audio.at[other], got_audio.at[me]),
        2: (lambda other: audio.at[mirror_of(other), 3], got_audio_query.at[me]),
        3: (lambda other: video_self.at[other], got_self.at[:, me]),
        4: (lambda other: video_far.at[other, 0], got_query.at[me]),
    }

    def send_all(*kinds):
        for j in kinds:
            pltpu.make_async_copy(spread[j][0](me), spread[j][1], arrived.at[j]).start()

        for j in kinds:

            def send(i, carry, j=j):
                other = partner(i)

                @pl.when(other != me)
                def _():
                    copy_to(spread[j][0](other), spread[j][1], j, other).start()

                return carry

            lax.fori_loop(0, count, send, 0)

    send_all(1)
    send_all(2)
    send_all(3)

    def wait_whole(ref, sem):
        pltpu.make_async_copy(ref, ref, sem).wait()

    step_gates = timestep[0]

    def gate(row, device):
        head = lax.rem(device, head_count)
        return gates[pl.ds(step_gates, 1), row, pl.ds(head, 1), :].reshape(1, head_size)

    wait_whole(got_audio, arrived.at[1])
    wait_whole(got_audio_query, arrived.at[2])
    for j in range(6):
        audio_sets[j] = got_audio[:, j].reshape(audio_total, head_size)
    audio_sets[6] = got_audio_query[...].reshape(audio_total, head_size)
    wait_whole(got_kv, arrived.at[0])

    block = audio_total // AUDIO_BLOCKS
    first_near = lax.rem(my_chip - chips // 4 + my_core + chips, chips) * 2 * video_rows
    position = first_near + lax.broadcasted_iota(jnp.int32, (half * video_rows, block), 0)
    position = jnp.where(
        position >= count * video_rows, position - count * video_rows, position
    )

    def rows_of(ref):
        return ref[...].reshape(-1, head_size)

    def cross_part(i, carry):
        kind, b = lax.div(i, AUDIO_BLOCKS), lax.rem(i, AUDIO_BLOCKS)
        pair = lax.rem(me + kind * half, count)
        side = lax.div(pair, half)
        found, level = attend_part(
            audio_sets[3 + 3 * kind, pl.ds(pl.multiple_of(b * block, block), block)],
            rows_of(got_kv.at[side, 0]),
            rows_of(got_kv.at[side, 1]),
            position < lengths[0, lax.div(pair, head_count)],
            scale,
        )
        half_found[i] = found
        half_stats[i] = level
        return carry

    lax.fori_loop(0, 2 * AUDIO_BLOCKS, cross_part, 0)
    stats_copy = pltpu.make_async_remote_copy(
        src_ref=half_stats,
        dst_ref=got_stats,
        send_sem=stats_sent,
        recv_sem=stats_arrived,
        device_id={"seq": mirror},
        device_id_type=MESH,
    )
    stats_copy.start()
    send_all(4)

    my_clip = lax.div(me, head_count)
    audio_visible = (
        lax.broadcasted_iota(jnp.int32, (1, audio_total), 1) < lengths[1, my_clip]
    )
    video_visible = (
        lax.broadcasted_iota(jnp.int32, (1, count * video_rows), 1) < lengths[0, my_clip]
    )

    def audio_block(b, carry):
        here = pl.ds(pl.multiple_of(b * block, block), block)
        own = attend(audio_sets[0, here], audio_sets[1], audio_sets[2], audio_visible, scale)
        part_audio[0, here] = gate(2, me) * own
        part_audio[1, here] = jnp.zeros_like(own)
        return carry

    lax.fori_loop(0, AUDIO_BLOCKS, audio_block, 0)

    stats_copy.wait()

    def join_parts(i, carry):
        kind, b = lax.div(i, AUDIO_BLOCKS), lax.rem(i, AUDIO_BLOCKS)
        pair = lax.rem(me + kind * half, count)
        above = got_stats[(1 - kind) * AUDIO_BLOCKS + b] - half_stats[i]
        weight = jnp.where(above < 80.0, 1.0 / (1.0 + jnp.exp(jnp.minimum(above, 80.0))), 0.0)
        found = half_found[i] * weight
        here = pl.ds(pl.multiple_of(b * block, block), block)
        part_audio[kind, here] = part_audio[kind, here] + gate(3, pair) * found.T
        return carry

    lax.fori_loop(0, 2 * AUDIO_BLOCKS, join_parts, 0)
    for kind in range(2):
        side = lax.rem(my_half + kind, 2)
        made_audio[side] = (
            part_audio[kind]
            .astype(jnp.bfloat16)
            .reshape(count, audio_rows // HALF_TILE, HALF_TILE, head_size)
        )

    def send_output(made, place, j, other):
        @pl.when(other != me)
        def _():
            pltpu.make_async_remote_copy(
                src_ref=made,
                dst_ref=place,
                send_sem=out_sent.at[j],
                recv_sem=out_arrived.at[j],
                device_id={"seq": other},
                device_id_type=MESH,
            ).start()

        @pl.when(other == me)
        def _():
            pltpu.make_async_copy(made, place, out_arrived.at[j]).start()

    def video_self_block(b, carry):
        here = pl.ds(b * Q_DEVICES, Q_DEVICES)
        own = attend(
            rows_of(got_self.at[0, here]),
            rows_of(got_self.at[1]),
            rows_of(got_self.at[2]),
            video_visible,
            scale,
        )
        part_video[here] = (gate(0, me) * own).reshape(Q_DEVICES, video_rows, head_size)
        return carry

    def send_audio(i, carry):
        other = partner(i)
        send_output(made_audio.at[:, other], got_made_audio.at[my_half, :, my_place], 1, other)
        return carry

    lax.fori_loop(0, count, send_audio, 0)

    wait_whole(got_self, arrived.at[3])
    lax.fori_loop(0, count // Q_DEVICES, video_self_block, 0)

    wait_whole(got_query, arrived.at[4])

    def video_cross_block(b, carry):
        blocks = count // Q_DEVICES
        offset = (blocks // 2 - lax.div(b + 1, 2)) * (1 - 2 * lax.rem(b, 2))
        first = lax.rem(lax.div(me, Q_DEVICES) + offset + blocks, blocks) * Q_DEVICES
        here = pl.ds(first, Q_DEVICES)
        far = attend(
            rows_of(got_query.at[here]), audio_sets[4], audio_sets[5], audio_visible, scale
        )
        mixed = part_video[here] + (gate(1, me) * far).reshape(Q_DEVICES, video_rows, head_size)
        made_video[here] = mixed.astype(jnp.bfloat16)

        def send(k, carry):
            other = first + k
            send_output(made_video.at[other], video_out.at[me], 0, other)
            return carry

        lax.fori_loop(0, Q_DEVICES, send, 0)
        return carry

    lax.fori_loop(0, count // Q_DEVICES, video_cross_block, 0)

    wait_whole(got_made_audio, out_arrived.at[1])
    whole_audio = got_made_audio[0].astype(jnp.float32) + got_made_audio[1].astype(jnp.float32)
    whole_audio = whole_audio.reshape(count // head_count, head_count, audio_rows, head_size)
    for clip in range(count // head_count):
        final_audio[clip] = jnp.swapaxes(whole_audio[clip], 0, 1).astype(jnp.bfloat16)
    keep_audio = pltpu.make_async_copy(final_audio, audio_out, loaded.at[0])
    keep_audio.start()
    keep_audio.wait()

    others = pl.ds(0, count - 1)
    wait_whole(video_far_halves.at[:, pl.ds(0, half - 1), keys_values], sent.at[0])
    wait_whole(audio.at[others], sent.at[1])
    wait_whole(audio.at[others, 3], sent.at[2])
    wait_whole(video_self.at[others], sent.at[3])
    wait_whole(video_far.at[others, 0], sent.at[4])
    wait_whole(made_video.at[others], out_sent.at[0])
    wait_whole(made_audio.at[:, others], out_sent.at[1])
    wait_whole(video_out, out_arrived.at[0])


def on_device(video_qkv, video_cross, audio_qkv, audio_cross, lengths, timestep, gate_table):
    count = lax.axis_size("seq")
    half = count // 2
    clip_count, head_count = video_qkv.shape[:2]
    video_rows, head_size = video_qkv.shape[3:]
    audio_rows = audio_qkv.shape[3]
    if clip_count * head_count != count or audio_rows % HALF_TILE:
        raise ValueError("unexpected shapes")
    quarters = audio_rows // HALF_TILE
    audio_total = count * audio_rows
    block = audio_total // AUDIO_BLOCKS

    video_self = video_qkv.reshape(count, 3, video_rows, head_size)
    video_far = video_cross.reshape(count, 3, video_rows, head_size)
    video_far_halves = video_cross.reshape(2, half, 3, video_rows, head_size)

    def heads_inside(tensor):
        return jnp.transpose(tensor, (0, 2, 3, 1, 4))

    bf16, f32 = jnp.bfloat16, jnp.float32
    anywhere = pl.BlockSpec(memory_space=pl.ANY)
    video_out, audio_out = pl.pallas_call(
        functools.partial(exchange_and_attend, head_count),
        out_shape=(
            jax.ShapeDtypeStruct((count, video_rows, head_size), bf16),
            jax.ShapeDtypeStruct((clip_count, audio_rows, head_count, head_size), bf16),
        ),
        in_specs=[pl.BlockSpec(memory_space=pltpu.SMEM)]
        + [pl.BlockSpec(memory_space=pltpu.HBM)] * 7,
        out_specs=[anywhere] * 2,
        scratch_shapes=[
            pltpu.SMEM(lengths.shape, lengths.dtype),
            pltpu.VMEM(gate_table.shape, f32),
            pltpu.VMEM((2, clip_count, 3, audio_rows, head_count, head_size), bf16),
            pltpu.VMEM((count, 6, quarters, HALF_TILE, head_size), bf16),
            pltpu.VMEM((3, count, video_rows, head_size), bf16),
            pltpu.VMEM((count, video_rows, head_size), bf16),
            pltpu.VMEM((2, 2, half, video_rows, head_size), bf16),
            pltpu.VMEM((count, 6, quarters, HALF_TILE, head_size), bf16),
            pltpu.VMEM((count, quarters, HALF_TILE, head_size), bf16),
            pltpu.VMEM((7, audio_total, head_size), bf16),
            pltpu.VMEM((count, video_rows, head_size), f32),
            pltpu.VMEM((count, video_rows, head_size), bf16),
            pltpu.VMEM((2, audio_total, head_size), f32),
            pltpu.VMEM((2 * AUDIO_BLOCKS, head_size, block), f32),
            pltpu.VMEM((2 * AUDIO_BLOCKS, 1, block), f32),
            pltpu.VMEM((2 * AUDIO_BLOCKS, 1, block), f32),
            pltpu.VMEM((2, count, quarters, HALF_TILE, head_size), bf16),
            pltpu.VMEM((2, 2, half, quarters, HALF_TILE, head_size), bf16),
            pltpu.VMEM((clip_count, audio_rows, head_count, head_size), bf16),
            pltpu.SemaphoreType.REGULAR((int(math.log2(half)) - 1,)),
            pltpu.SemaphoreType.DMA((4,)),
            pltpu.SemaphoreType.DMA((5,)),
            pltpu.SemaphoreType.DMA((5,)),
            pltpu.SemaphoreType.DMA,
            pltpu.SemaphoreType.DMA,
            pltpu.SemaphoreType.DMA((2,)),
            pltpu.SemaphoreType.DMA((2,)),
        ],
        compiler_params=pltpu.CompilerParams(
            collective_id=0, has_side_effects=True, vmem_limit_bytes=40 * 2**20
        ),
    )(
        timestep,
        *(
            pltpu.with_memory_space_constraint(tensor, pltpu.HBM)
            for tensor in (
                lengths,
                gate_table,
                video_self,
                video_far,
                video_far_halves,
                heads_inside(audio_qkv),
                heads_inside(audio_cross),
            )
        ),
    )
    return (
        video_out.reshape(clip_count, head_count, video_rows, head_size),
        jnp.swapaxes(audio_out, 1, 2),
    )


def solution(mesh):
    tokens = P("groups", None, None, "seq", None)
    made = P("groups", None, "seq", None)
    return jax.shard_map(
        on_device,
        mesh=mesh,
        in_specs=(tokens, tokens, tokens, tokens, P(None, "groups"), P("groups"), P()),
        out_specs=(made, made),
        check_vma=False,
    )
```

```python
import functools
import math

import jax
import jax.numpy as jnp
from jax import lax
from jax.experimental import pallas as pl
from jax.experimental.pallas import tpu as pltpu
from jax.sharding import PartitionSpec as P

MESH = pl.DeviceIdType.MESH
HALF_TILE = 4
Q_DEVICES = 4
AUDIO_BLOCKS = 3
FIRST_REACH = 4


def dot_rows(left, right):
    return lax.dot_general(
        left, right, (((1,), (1,)), ((), ())), preferred_element_type=jnp.float32
    )


def attend(queries, key_rows, values, visible, scale):
    scores = jnp.where(visible, dot_rows(queries, key_rows) * scale, -1e30)
    row_max = jnp.max(scores, axis=1, keepdims=True)
    weights = jnp.exp(scores - row_max)
    row_total = jnp.sum(weights, axis=1, keepdims=True)
    found = jnp.dot(weights.astype(jnp.bfloat16), values, preferred_element_type=jnp.float32)
    return found / row_total


def attend_part(queries, key_rows, values, visible, scale):
    scores = jnp.where(visible, dot_rows(key_rows, queries) * scale, -1e30)
    top = jnp.max(scores, axis=0, keepdims=True)
    weights = jnp.exp(scores - top)
    total = jnp.sum(weights, axis=0, keepdims=True)
    found = lax.dot_general(
        values,
        weights.astype(jnp.bfloat16),
        (((0,), (0,)), ((), ())),
        preferred_element_type=jnp.float32,
    )
    return found / total, top + jnp.log(total)


def exchange_and_attend(
    head_count,
    timestep,
    lengths_given,
    gate_table,
    video_self,
    video_far,
    video_far_halves,
    audio_self_raw,
    audio_far_raw,
    video_out,
    audio_out,
    lengths,
    gates,
    raw,
    audio,
    got_self,
    got_query,
    got_kv,
    got_audio,
    got_audio_query,
    audio_sets,
    part_video,
    made_video,
    part_audio,
    half_found,
    half_stats,
    got_stats,
    made_audio,
    got_made_audio,
    final_audio,
    known,
    loaded,
    sent,
    arrived,
    stats_sent,
    stats_arrived,
    out_sent,
    out_arrived,
):
    me = lax.axis_index("seq")
    count = got_self.shape[1]
    half = count // 2
    chips = count // 2
    head_size = got_self.shape[3]
    video_rows = got_self.shape[2]
    audio_rows = raw.shape[3]
    audio_total = count * audio_rows
    scale = 1.0 / math.sqrt(head_size)
    my_chip, my_core = lax.div(me, 2), lax.rem(me, 2)
    mirror = lax.rem(me + half, count)
    my_half, my_place = lax.div(me, half), lax.rem(me, half)

    def at_offset(offset, core):
        return lax.rem(my_chip + offset + chips, chips) * 2 + core

    def partner(i):
        step = lax.div(i, 2)
        offset = (chips // 2 - lax.div(step + 1, 2)) * (1 - 2 * lax.rem(step, 2))
        return at_offset(offset, lax.rem(my_core + lax.rem(i, 2), 2))

    def near_target(i):
        step, core = lax.div(i, 2), lax.rem(i, 2)
        offset = (chips // 4 - lax.div(step + 1, 2)) * (1 - 2 * lax.rem(step, 2)) * (1 - 2 * core)
        slot = (chips // 4 - core - offset) * 2 + my_core
        return at_offset(offset, core), slot

    loads = (
        pltpu.make_async_copy(audio_self_raw, raw.at[0], loaded.at[0]),
        pltpu.make_async_copy(audio_far_raw, raw.at[1], loaded.at[1]),
        pltpu.make_async_copy(gate_table, gates, loaded.at[2]),
        pltpu.make_async_copy(lengths_given, lengths, loaded.at[3]),
    )
    for load in loads:
        load.start()

    barrier = pltpu.get_barrier_semaphore()

    def greet(i, carry):
        other = at_offset(lax.div(i, 2) - FIRST_REACH, lax.rem(i, 2))

        @pl.when(other != me)
        def _():
            pl.semaphore_signal(barrier, inc=1, device_id={"seq": other}, device_id_type=MESH)

        return carry

    lax.fori_loop(0, 4 * FIRST_REACH + 2, greet, 0)
    pl.semaphore_wait(barrier, 4 * FIRST_REACH + 1)

    def pass_on(step, distance):
        for offset in (-distance, distance):
            pl.semaphore_signal(
                known.at[step],
                inc=1,
                device_id={"seq": at_offset(offset, my_core)},
                device_id_type=MESH,
            )

    keys_values = pl.ds(1, 2)

    def copy_to(source, place, j, other):
        return pltpu.make_async_remote_copy(
            src_ref=source,
            dst_ref=place,
            send_sem=sent.at[j],
            recv_sem=arrived.at[j],
            device_id={"seq": other},
            device_id_type=MESH,
        )

    def send_kv(i, carry):
        other, slot = near_target(i)
        source = video_far_halves.at[:, lax.rem(other, half), keys_values]
        place = got_kv.at[:, :, slot]

        @pl.when(other != me)
        def _():
            copy_to(source, place, 0, other).start()

        @pl.when(other == me)
        def _():
            pltpu.make_async_copy(source, place, arrived.at[0]).start()

        return carry

    quarter = chips // 4
    reach, unsent = FIRST_REACH, half
    for step in range(known.shape[0]):
        pass_on(step, reach)
        start = max(0, 4 * (quarter - reach) - 2)
        lax.fori_loop(start, unsent, send_kv, 0)
        unsent, reach = start, 2 * reach
        if step < known.shape[0] - 1:
            pl.semaphore_wait(known.at[step], 2)

    for load in loads:
        load.wait()
    for side in range(2):
        for clip in range(raw.shape[1]):
            rows = raw[side, clip].astype(jnp.float32)
            rows = rows.reshape(3 * audio_rows, head_count, head_size)
            rows = jnp.swapaxes(rows, 0, 1).astype(jnp.bfloat16)
            audio[pl.ds(clip * head_count, head_count), pl.ds(3 * side, 3)] = rows.reshape(
                head_count, 3, audio_rows // HALF_TILE, HALF_TILE, head_size
            )

    pl.semaphore_wait(known.at[known.shape[0] - 1], 2)

    def mirror_of(device):
        return lax.rem(device + half, count)

    spread = {
        1: (lambda other: audio.at[other], got_audio.at[me]),
        2: (lambda other: audio.at[mirror_of(other), 3], got_audio_query.at[me]),
        3: (lambda other: video_self.at[other], got_self.at[:, me]),
        4: (lambda other: video_far.at[other, 0], got_query.at[me]),
    }

    def send_all(*kinds):
        for j in kinds:
            pltpu.make_async_copy(spread[j][0](me), spread[j][1], arrived.at[j]).start()

        for j in kinds:

            def send(i, carry, j=j):
                other = partner(i)

                @pl.when(other != me)
                def _():
                    copy_to(spread[j][0](other), spread[j][1], j, other).start()

                return carry

            lax.fori_loop(0, count, send, 0)

    send_all(1)
    send_all(2)
    send_all(3)

    def wait_whole(ref, sem):
        pltpu.make_async_copy(ref, ref, sem).wait()

    step_gates = timestep[0]

    def gate(row, device):
        head = lax.rem(device, head_count)
        return gates[pl.ds(step_gates, 1), row, pl.ds(head, 1), :].reshape(1, head_size)

    wait_whole(got_audio, arrived.at[1])
    wait_whole(got_audio_query, arrived.at[2])
    for j in range(6):
        audio_sets[j] = got_audio[:, j].reshape(audio_total, head_size)
    audio_sets[6] = got_audio_query[...].reshape(audio_total, head_size)
    wait_whole(got_kv, arrived.at[0])

    block = audio_total // AUDIO_BLOCKS
    first_near = lax.rem(my_chip - chips // 4 + my_core + chips, chips) * 2 * video_rows
    position = first_near + lax.broadcasted_iota(jnp.int32, (half * video_rows, block), 0)
    position = jnp.where(
        position >= count * video_rows, position - count * video_rows, position
    )

    def rows_of(ref):
        return ref[...].reshape(-1, head_size)

    def cross_part(i, carry):
        kind, b = lax.div(i, AUDIO_BLOCKS), lax.rem(i, AUDIO_BLOCKS)
        pair = lax.rem(me + kind * half, count)
        side = lax.div(pair, half)
        found, level = attend_part(
            audio_sets[3 + 3 * kind, pl.ds(pl.multiple_of(b * block, block), block)],
            rows_of(got_kv.at[side, 0]),
            rows_of(got_kv.at[side, 1]),
            position < lengths[0, lax.div(pair, head_count)],
            scale,
        )
        half_found[i] = found
        half_stats[i] = level
        return carry

    lax.fori_loop(0, 2 * AUDIO_BLOCKS, cross_part, 0)
    stats_copy = pltpu.make_async_remote_copy(
        src_ref=half_stats,
        dst_ref=got_stats,
        send_sem=stats_sent,
        recv_sem=stats_arrived,
        device_id={"seq": mirror},
        device_id_type=MESH,
    )
    stats_copy.start()
    send_all(4)

    my_clip = lax.div(me, head_count)
    audio_visible = (
        lax.broadcasted_iota(jnp.int32, (1, audio_total), 1) < lengths[1, my_clip]
    )
    video_visible = (
        lax.broadcasted_iota(jnp.int32, (1, count * video_rows), 1) < lengths[0, my_clip]
    )

    def audio_block(b, carry):
        here = pl.ds(pl.multiple_of(b * block, block), block)
        own = attend(audio_sets[0, here], audio_sets[1], audio_sets[2], audio_visible, scale)
        part_audio[0, here] = gate(2, me) * own
        part_audio[1, here] = jnp.zeros_like(own)
        return carry

    lax.fori_loop(0, AUDIO_BLOCKS, audio_block, 0)

    stats_copy.wait()

    def join_parts(i, carry):
        kind, b = lax.div(i, AUDIO_BLOCKS), lax.rem(i, AUDIO_BLOCKS)
        pair = lax.rem(me + kind * half, count)
        above = got_stats[(1 - kind) * AUDIO_BLOCKS + b] - half_stats[i]
        weight = jnp.where(above < 80.0, 1.0 / (1.0 + jnp.exp(jnp.minimum(above, 80.0))), 0.0)
        found = half_found[i] * weight
        here = pl.ds(pl.multiple_of(b * block, block), block)
        part_audio[kind, here] = part_audio[kind, here] + gate(3, pair) * found.T
        return carry

    lax.fori_loop(0, 2 * AUDIO_BLOCKS, join_parts, 0)
    for kind in range(2):
        side = lax.rem(my_half + kind, 2)
        made_audio[side] = (
            part_audio[kind]
            .astype(jnp.bfloat16)
            .reshape(count, audio_rows // HALF_TILE, HALF_TILE, head_size)
        )

    def send_output(made, place, j, other):
        @pl.when(other != me)
        def _():
            pltpu.make_async_remote_copy(
                src_ref=made,
                dst_ref=place,
                send_sem=out_sent.at[j],
                recv_sem=out_arrived.at[j],
                device_id={"seq": other},
                device_id_type=MESH,
            ).start()

        @pl.when(other == me)
        def _():
            pltpu.make_async_copy(made, place, out_arrived.at[j]).start()

    def video_self_block(b, carry):
        here = pl.ds(b * Q_DEVICES, Q_DEVICES)
        own = attend(
            rows_of(got_self.at[0, here]),
            rows_of(got_self.at[1]),
            rows_of(got_self.at[2]),
            video_visible,
            scale,
        )
        part_video[here] = (gate(0, me) * own).reshape(Q_DEVICES, video_rows, head_size)
        return carry

    def send_audio(i, carry):
        other = partner(i)
        send_output(made_audio.at[:, other], got_made_audio.at[my_half, :, my_place], 1, other)
        return carry

    lax.fori_loop(0, count, send_audio, 0)

    wait_whole(got_self, arrived.at[3])
    lax.fori_loop(0, count // Q_DEVICES, video_self_block, 0)

    wait_whole(got_query, arrived.at[4])

    def video_cross_block(b, carry):
        blocks = count // Q_DEVICES
        offset = (blocks // 2 - lax.div(b + 1, 2)) * (1 - 2 * lax.rem(b, 2))
        first = lax.rem(lax.div(me, Q_DEVICES) + offset + blocks, blocks) * Q_DEVICES
        here = pl.ds(first, Q_DEVICES)
        far = attend(
            rows_of(got_query.at[here]), audio_sets[4], audio_sets[5], audio_visible, scale
        )
        mixed = part_video[here] + (gate(1, me) * far).reshape(Q_DEVICES, video_rows, head_size)
        made_video[here] = mixed.astype(jnp.bfloat16)

        def send(k, carry):
            other = first + k
            send_output(made_video.at[other], video_out.at[me], 0, other)
            return carry

        lax.fori_loop(0, Q_DEVICES, send, 0)
        return carry

    lax.fori_loop(0, count // Q_DEVICES, video_cross_block, 0)

    wait_whole(got_made_audio, out_arrived.at[1])
    whole_audio = got_made_audio[0].astype(jnp.float32) + got_made_audio[1].astype(jnp.float32)
    whole_audio = whole_audio.reshape(count // head_count, head_count, audio_rows, head_size)
    for clip in range(count // head_count):
        final_audio[clip] = jnp.swapaxes(whole_audio[clip], 0, 1).astype(jnp.bfloat16)
    keep_audio = pltpu.make_async_copy(final_audio, audio_out, loaded.at[0])
    keep_audio.start()
    keep_audio.wait()

    others = pl.ds(0, count - 1)
    wait_whole(video_far_halves.at[:, pl.ds(0, half - 1), keys_values], sent.at[0])
    wait_whole(audio.at[others], sent.at[1])
    wait_whole(audio.at[others, 3], sent.at[2])
    wait_whole(video_self.at[others], sent.at[3])
    wait_whole(video_far.at[others, 0], sent.at[4])
    wait_whole(made_video.at[others], out_sent.at[0])
    wait_whole(made_audio.at[:, others], out_sent.at[1])
    wait_whole(video_out, out_arrived.at[0])


def on_device(video_qkv, video_cross, audio_qkv, audio_cross, lengths, timestep, gate_table):
    count = lax.axis_size("seq")
    half = count // 2
    clip_count, head_count = video_qkv.shape[:2]
    video_rows, head_size = video_qkv.shape[3:]
    audio_rows = audio_qkv.shape[3]
    if clip_count * head_count != count or audio_rows % HALF_TILE:
        raise ValueError("unexpected shapes")
    quarters = audio_rows // HALF_TILE
    audio_total = count * audio_rows
    block = audio_total // AUDIO_BLOCKS

    video_self = video_qkv.reshape(count, 3, video_rows, head_size)
    video_far = video_cross.reshape(count, 3, video_rows, head_size)
    video_far_halves = video_cross.reshape(2, half, 3, video_rows, head_size)

    def heads_inside(tensor):
        return jnp.transpose(tensor, (0, 2, 3, 1, 4))

    bf16, f32 = jnp.bfloat16, jnp.float32
    anywhere = pl.BlockSpec(memory_space=pl.ANY)
    video_out, audio_out = pl.pallas_call(
        functools.partial(exchange_and_attend, head_count),
        out_shape=(
            jax.ShapeDtypeStruct((count, video_rows, head_size), bf16),
            jax.ShapeDtypeStruct((clip_count, audio_rows, head_count, head_size), bf16),
        ),
        in_specs=[pl.BlockSpec(memory_space=pltpu.SMEM)]
        + [pl.BlockSpec(memory_space=pltpu.HBM)] * 7,
        out_specs=[anywhere] * 2,
        scratch_shapes=[
            pltpu.SMEM(lengths.shape, lengths.dtype),
            pltpu.VMEM(gate_table.shape, f32),
            pltpu.VMEM((2, clip_count, 3, audio_rows, head_count, head_size), bf16),
            pltpu.VMEM((count, 6, quarters, HALF_TILE, head_size), bf16),
            pltpu.VMEM((3, count, video_rows, head_size), bf16),
            pltpu.VMEM((count, video_rows, head_size), bf16),
            pltpu.VMEM((2, 2, half, video_rows, head_size), bf16),
            pltpu.VMEM((count, 6, quarters, HALF_TILE, head_size), bf16),
            pltpu.VMEM((count, quarters, HALF_TILE, head_size), bf16),
            pltpu.VMEM((7, audio_total, head_size), bf16),
            pltpu.VMEM((count, video_rows, head_size), f32),
            pltpu.VMEM((count, video_rows, head_size), bf16),
            pltpu.VMEM((2, audio_total, head_size), f32),
            pltpu.VMEM((2 * AUDIO_BLOCKS, head_size, block), f32),
            pltpu.VMEM((2 * AUDIO_BLOCKS, 1, block), f32),
            pltpu.VMEM((2 * AUDIO_BLOCKS, 1, block), f32),
            pltpu.VMEM((2, count, quarters, HALF_TILE, head_size), bf16),
            pltpu.VMEM((2, 2, half, quarters, HALF_TILE, head_size), bf16),
            pltpu.VMEM((clip_count, audio_rows, head_count, head_size), bf16),
            pltpu.SemaphoreType.REGULAR((int(math.log2(half // 2 // FIRST_REACH)),)),
            pltpu.SemaphoreType.DMA((4,)),
            pltpu.SemaphoreType.DMA((5,)),
            pltpu.SemaphoreType.DMA((5,)),
            pltpu.SemaphoreType.DMA,
            pltpu.SemaphoreType.DMA,
            pltpu.SemaphoreType.DMA((2,)),
            pltpu.SemaphoreType.DMA((2,)),
        ],
        compiler_params=pltpu.CompilerParams(
            collective_id=0, has_side_effects=True, vmem_limit_bytes=40 * 2**20
        ),
    )(
        timestep,
        *(
            pltpu.with_memory_space_constraint(tensor, pltpu.HBM)
            for tensor in (
                lengths,
                gate_table,
                video_self,
                video_far,
                video_far_halves,
                heads_inside(audio_qkv),
                heads_inside(audio_cross),
            )
        ),
    )
    return (
        video_out.reshape(clip_count, head_count, video_rows, head_size),
        jnp.swapaxes(audio_out, 1, 2),
    )


def solution(mesh):
    tokens = P("groups", None, None, "seq", None)
    made = P("groups", None, "seq", None)
    return jax.shard_map(
        on_device,
        mesh=mesh,
        in_specs=(tokens, tokens, tokens, tokens, P(None, "groups"), P("groups"), P()),
        out_specs=(made, made),
        check_vma=False,
    )
```

```python
import functools
import math

import jax
import jax.numpy as jnp
from jax import lax
from jax.experimental import pallas as pl
from jax.experimental.pallas import tpu as pltpu
from jax.sharding import PartitionSpec as P

MESH = pl.DeviceIdType.MESH
HALF_TILE = 4
Q_DEVICES = 4
AUDIO_BLOCKS = 3
FIRST_REACH = 2


def dot_rows(left, right):
    return lax.dot_general(
        left, right, (((1,), (1,)), ((), ())), preferred_element_type=jnp.float32
    )


def attend(queries, key_rows, values, visible, scale):
    scores = jnp.where(visible, dot_rows(queries, key_rows) * scale, -1e30)
    row_max = jnp.max(scores, axis=1, keepdims=True)
    weights = jnp.exp(scores - row_max)
    row_total = jnp.sum(weights, axis=1, keepdims=True)
    found = jnp.dot(weights.astype(jnp.bfloat16), values, preferred_element_type=jnp.float32)
    return found / row_total


def attend_part(queries, key_rows, values, visible, scale):
    scores = jnp.where(visible, dot_rows(key_rows, queries) * scale, -1e30)
    top = jnp.max(scores, axis=0, keepdims=True)
    weights = jnp.exp(scores - top)
    total = jnp.sum(weights, axis=0, keepdims=True)
    found = lax.dot_general(
        values,
        weights.astype(jnp.bfloat16),
        (((0,), (0,)), ((), ())),
        preferred_element_type=jnp.float32,
    )
    return found / total, top + jnp.log(total)


def exchange_and_attend(
    head_count,
    timestep,
    lengths_given,
    gate_table,
    video_self,
    video_far,
    video_far_halves,
    audio_self_raw,
    audio_far_raw,
    video_out,
    audio_out,
    lengths,
    gates,
    raw,
    audio,
    got_self,
    got_query,
    got_kv,
    got_audio,
    got_audio_query,
    audio_sets,
    part_video,
    made_video,
    part_audio,
    half_found,
    half_stats,
    got_stats,
    made_audio,
    got_made_audio,
    final_audio,
    known,
    loaded,
    sent,
    arrived,
    stats_sent,
    stats_arrived,
    out_sent,
    out_arrived,
):
    me = lax.axis_index("seq")
    count = got_self.shape[1]
    half = count // 2
    chips = count // 2
    head_size = got_self.shape[3]
    video_rows = got_self.shape[2]
    audio_rows = raw.shape[3]
    audio_total = count * audio_rows
    scale = 1.0 / math.sqrt(head_size)
    my_chip, my_core = lax.div(me, 2), lax.rem(me, 2)
    mirror = lax.rem(me + half, count)
    my_half, my_place = lax.div(me, half), lax.rem(me, half)

    def at_offset(offset, core):
        return lax.rem(my_chip + offset + chips, chips) * 2 + core

    def partner(i):
        step = lax.div(i, 2)
        offset = (chips // 2 - lax.div(step + 1, 2)) * (1 - 2 * lax.rem(step, 2))
        return at_offset(offset, lax.rem(my_core + lax.rem(i, 2), 2))

    def near_target(i):
        step, core = lax.div(i, 2), lax.rem(i, 2)
        offset = (chips // 4 - lax.div(step + 1, 2)) * (1 - 2 * lax.rem(step, 2)) * (1 - 2 * core)
        slot = (chips // 4 - core - offset) * 2 + my_core
        return at_offset(offset, core), slot

    loads = (
        pltpu.make_async_copy(audio_self_raw, raw.at[0], loaded.at[0]),
        pltpu.make_async_copy(audio_far_raw, raw.at[1], loaded.at[1]),
        pltpu.make_async_copy(gate_table, gates, loaded.at[2]),
        pltpu.make_async_copy(lengths_given, lengths, loaded.at[3]),
    )
    for load in loads:
        load.start()

    barrier = pltpu.get_barrier_semaphore()

    def greet(i, carry):
        other = at_offset(lax.div(i, 2) - FIRST_REACH, lax.rem(i, 2))

        @pl.when(other != me)
        def _():
            pl.semaphore_signal(barrier, inc=1, device_id={"seq": other}, device_id_type=MESH)

        return carry

    lax.fori_loop(0, 4 * FIRST_REACH + 2, greet, 0)
    pl.semaphore_wait(barrier, 4 * FIRST_REACH + 1)

    def pass_on(step, distance):
        for offset in (-distance, distance):
            pl.semaphore_signal(
                known.at[step],
                inc=1,
                device_id={"seq": at_offset(offset, my_core)},
                device_id_type=MESH,
            )

    keys_values = pl.ds(1, 2)

    def copy_to(source, place, j, other):
        return pltpu.make_async_remote_copy(
            src_ref=source,
            dst_ref=place,
            send_sem=sent.at[j],
            recv_sem=arrived.at[j],
            device_id={"seq": other},
            device_id_type=MESH,
        )

    def send_kv(i, carry):
        other, slot = near_target(i)
        source = video_far_halves.at[:, lax.rem(other, half), keys_values]
        place = got_kv.at[:, :, slot]

        @pl.when(other != me)
        def _():
            copy_to(source, place, 0, other).start()

        @pl.when(other == me)
        def _():
            pltpu.make_async_copy(source, place, arrived.at[0]).start()

        return carry

    quarter = chips // 4
    reach, unsent = FIRST_REACH, half
    for step in range(known.shape[0]):
        pass_on(step, reach)
        start = max(0, 4 * (quarter - reach) - 2)
        lax.fori_loop(start, unsent, send_kv, 0)
        unsent, reach = start, 2 * reach
        if step < known.shape[0] - 1:
            pl.semaphore_wait(known.at[step], 2)

    for load in loads:
        load.wait()
    for side in range(2):
        for clip in range(raw.shape[1]):
            rows = raw[side, clip].astype(jnp.float32)
            rows = rows.reshape(3 * audio_rows, head_count, head_size)
            rows = jnp.swapaxes(rows, 0, 1).astype(jnp.bfloat16)
            audio[pl.ds(clip * head_count, head_count), pl.ds(3 * side, 3)] = rows.reshape(
                head_count, 3, audio_rows // HALF_TILE, HALF_TILE, head_size
            )

    pl.semaphore_wait(known.at[known.shape[0] - 1], 2)

    def mirror_of(device):
        return lax.rem(device + half, count)

    spread = {
        1: (lambda other: audio.at[other], got_audio.at[me]),
        2: (lambda other: audio.at[mirror_of(other), 3], got_audio_query.at[me]),
        3: (lambda other: video_self.at[other], got_self.at[:, me]),
        4: (lambda other: video_far.at[other, 0], got_query.at[me]),
    }

    def send_all(*kinds):
        for j in kinds:
            pltpu.make_async_copy(spread[j][0](me), spread[j][1], arrived.at[j]).start()

        for j in kinds:

            def send(i, carry, j=j):
                other = partner(i)

                @pl.when(other != me)
                def _():
                    copy_to(spread[j][0](other), spread[j][1], j, other).start()

                return carry

            lax.fori_loop(0, count, send, 0)

    send_all(1)
    send_all(2)
    send_all(3)

    def wait_whole(ref, sem):
        pltpu.make_async_copy(ref, ref, sem).wait()

    step_gates = timestep[0]

    def gate(row, device):
        head = lax.rem(device, head_count)
        return gates[pl.ds(step_gates, 1), row, pl.ds(head, 1), :].reshape(1, head_size)

    wait_whole(got_audio, arrived.at[1])
    wait_whole(got_audio_query, arrived.at[2])
    for j in range(6):
        audio_sets[j] = got_audio[:, j].reshape(audio_total, head_size)
    audio_sets[6] = got_audio_query[...].reshape(audio_total, head_size)
    wait_whole(got_kv, arrived.at[0])

    block = audio_total // AUDIO_BLOCKS
    first_near = lax.rem(my_chip - chips // 4 + my_core + chips, chips) * 2 * video_rows
    position = first_near + lax.broadcasted_iota(jnp.int32, (half * video_rows, block), 0)
    position = jnp.where(
        position >= count * video_rows, position - count * video_rows, position
    )

    def rows_of(ref):
        return ref[...].reshape(-1, head_size)

    def cross_part(i, carry):
        kind, b = lax.div(i, AUDIO_BLOCKS), lax.rem(i, AUDIO_BLOCKS)
        pair = lax.rem(me + kind * half, count)
        side = lax.div(pair, half)
        found, level = attend_part(
            audio_sets[3 + 3 * kind, pl.ds(pl.multiple_of(b * block, block), block)],
            rows_of(got_kv.at[side, 0]),
            rows_of(got_kv.at[side, 1]),
            position < lengths[0, lax.div(pair, head_count)],
            scale,
        )
        half_found[i] = found
        half_stats[i] = level
        return carry

    lax.fori_loop(0, 2 * AUDIO_BLOCKS, cross_part, 0)
    stats_copy = pltpu.make_async_remote_copy(
        src_ref=half_stats,
        dst_ref=got_stats,
        send_sem=stats_sent,
        recv_sem=stats_arrived,
        device_id={"seq": mirror},
        device_id_type=MESH,
    )
    stats_copy.start()
    send_all(4)

    my_clip = lax.div(me, head_count)
    audio_visible = (
        lax.broadcasted_iota(jnp.int32, (1, audio_total), 1) < lengths[1, my_clip]
    )
    video_visible = (
        lax.broadcasted_iota(jnp.int32, (1, count * video_rows), 1) < lengths[0, my_clip]
    )

    def audio_block(b, carry):
        here = pl.ds(pl.multiple_of(b * block, block), block)
        own = attend(audio_sets[0, here], audio_sets[1], audio_sets[2], audio_visible, scale)
        part_audio[0, here] = gate(2, me) * own
        part_audio[1, here] = jnp.zeros_like(own)
        return carry

    lax.fori_loop(0, AUDIO_BLOCKS, audio_block, 0)

    stats_copy.wait()

    def join_parts(i, carry):
        kind, b = lax.div(i, AUDIO_BLOCKS), lax.rem(i, AUDIO_BLOCKS)
        pair = lax.rem(me + kind * half, count)
        above = got_stats[(1 - kind) * AUDIO_BLOCKS + b] - half_stats[i]
        weight = jnp.where(above < 80.0, 1.0 / (1.0 + jnp.exp(jnp.minimum(above, 80.0))), 0.0)
        found = half_found[i] * weight
        here = pl.ds(pl.multiple_of(b * block, block), block)
        part_audio[kind, here] = part_audio[kind, here] + gate(3, pair) * found.T
        return carry

    lax.fori_loop(0, 2 * AUDIO_BLOCKS, join_parts, 0)
    for kind in range(2):
        side = lax.rem(my_half + kind, 2)
        made_audio[side] = (
            part_audio[kind]
            .astype(jnp.bfloat16)
            .reshape(count, audio_rows // HALF_TILE, HALF_TILE, head_size)
        )

    def send_output(made, place, j, other):
        @pl.when(other != me)
        def _():
            pltpu.make_async_remote_copy(
                src_ref=made,
                dst_ref=place,
                send_sem=out_sent.at[j],
                recv_sem=out_arrived.at[j],
                device_id={"seq": other},
                device_id_type=MESH,
            ).start()

        @pl.when(other == me)
        def _():
            pltpu.make_async_copy(made, place, out_arrived.at[j]).start()

    def video_self_block(b, carry):
        here = pl.ds(b * Q_DEVICES, Q_DEVICES)
        own = attend(
            rows_of(got_self.at[0, here]),
            rows_of(got_self.at[1]),
            rows_of(got_self.at[2]),
            video_visible,
            scale,
        )
        part_video[here] = (gate(0, me) * own).reshape(Q_DEVICES, video_rows, head_size)
        return carry

    def send_audio(i, carry):
        other = partner(i)
        send_output(made_audio.at[:, other], got_made_audio.at[my_half, :, my_place], 1, other)
        return carry

    lax.fori_loop(0, count, send_audio, 0)

    wait_whole(got_self, arrived.at[3])
    lax.fori_loop(0, count // Q_DEVICES, video_self_block, 0)

    wait_whole(got_query, arrived.at[4])

    def video_cross_block(b, carry):
        blocks = count // Q_DEVICES
        offset = (blocks // 2 - lax.div(b + 1, 2)) * (1 - 2 * lax.rem(b, 2))
        first = lax.rem(lax.div(me, Q_DEVICES) + offset + blocks, blocks) * Q_DEVICES
        here = pl.ds(first, Q_DEVICES)
        far = attend(
            rows_of(got_query.at[here]), audio_sets[4], audio_sets[5], audio_visible, scale
        )
        mixed = part_video[here] + (gate(1, me) * far).reshape(Q_DEVICES, video_rows, head_size)
        made_video[here] = mixed.astype(jnp.bfloat16)

        def send(k, carry):
            other = first + k
            send_output(made_video.at[other], video_out.at[me], 0, other)
            return carry

        lax.fori_loop(0, Q_DEVICES, send, 0)
        return carry

    lax.fori_loop(0, count // Q_DEVICES, video_cross_block, 0)

    wait_whole(got_made_audio, out_arrived.at[1])
    whole_audio = got_made_audio[0].astype(jnp.float32) + got_made_audio[1].astype(jnp.float32)
    whole_audio = whole_audio.reshape(count // head_count, head_count, audio_rows, head_size)
    for clip in range(count // head_count):
        final_audio[clip] = jnp.swapaxes(whole_audio[clip], 0, 1).astype(jnp.bfloat16)
    keep_audio = pltpu.make_async_copy(final_audio, audio_out, loaded.at[0])
    keep_audio.start()
    keep_audio.wait()

    others = pl.ds(0, count - 1)
    wait_whole(video_far_halves.at[:, pl.ds(0, half - 1), keys_values], sent.at[0])
    wait_whole(audio.at[others], sent.at[1])
    wait_whole(audio.at[others, 3], sent.at[2])
    wait_whole(video_self.at[others], sent.at[3])
    wait_whole(video_far.at[others, 0], sent.at[4])
    wait_whole(made_video.at[others], out_sent.at[0])
    wait_whole(made_audio.at[:, others], out_sent.at[1])
    wait_whole(video_out, out_arrived.at[0])


def on_device(video_qkv, video_cross, audio_qkv, audio_cross, lengths, timestep, gate_table):
    count = lax.axis_size("seq")
    half = count // 2
    clip_count, head_count = video_qkv.shape[:2]
    video_rows, head_size = video_qkv.shape[3:]
    audio_rows = audio_qkv.shape[3]
    if clip_count * head_count != count or audio_rows % HALF_TILE:
        raise ValueError("unexpected shapes")
    quarters = audio_rows // HALF_TILE
    audio_total = count * audio_rows
    block = audio_total // AUDIO_BLOCKS

    video_self = video_qkv.reshape(count, 3, video_rows, head_size)
    video_far = video_cross.reshape(count, 3, video_rows, head_size)
    video_far_halves = video_cross.reshape(2, half, 3, video_rows, head_size)

    def heads_inside(tensor):
        return jnp.transpose(tensor, (0, 2, 3, 1, 4))

    bf16, f32 = jnp.bfloat16, jnp.float32
    anywhere = pl.BlockSpec(memory_space=pl.ANY)
    video_out, audio_out = pl.pallas_call(
        functools.partial(exchange_and_attend, head_count),
        out_shape=(
            jax.ShapeDtypeStruct((count, video_rows, head_size), bf16),
            jax.ShapeDtypeStruct((clip_count, audio_rows, head_count, head_size), bf16),
        ),
        in_specs=[pl.BlockSpec(memory_space=pltpu.SMEM)]
        + [pl.BlockSpec(memory_space=pltpu.HBM)] * 7,
        out_specs=[anywhere] * 2,
        scratch_shapes=[
            pltpu.SMEM(lengths.shape, lengths.dtype),
            pltpu.VMEM(gate_table.shape, f32),
            pltpu.VMEM((2, clip_count, 3, audio_rows, head_count, head_size), bf16),
            pltpu.VMEM((count, 6, quarters, HALF_TILE, head_size), bf16),
            pltpu.VMEM((3, count, video_rows, head_size), bf16),
            pltpu.VMEM((count, video_rows, head_size), bf16),
            pltpu.VMEM((2, 2, half, video_rows, head_size), bf16),
            pltpu.VMEM((count, 6, quarters, HALF_TILE, head_size), bf16),
            pltpu.VMEM((count, quarters, HALF_TILE, head_size), bf16),
            pltpu.VMEM((7, audio_total, head_size), bf16),
            pltpu.VMEM((count, video_rows, head_size), f32),
            pltpu.VMEM((count, video_rows, head_size), bf16),
            pltpu.VMEM((2, audio_total, head_size), f32),
            pltpu.VMEM((2 * AUDIO_BLOCKS, head_size, block), f32),
            pltpu.VMEM((2 * AUDIO_BLOCKS, 1, block), f32),
            pltpu.VMEM((2 * AUDIO_BLOCKS, 1, block), f32),
            pltpu.VMEM((2, count, quarters, HALF_TILE, head_size), bf16),
            pltpu.VMEM((2, 2, half, quarters, HALF_TILE, head_size), bf16),
            pltpu.VMEM((clip_count, audio_rows, head_count, head_size), bf16),
            pltpu.SemaphoreType.REGULAR((int(math.log2(half // 2 // FIRST_REACH)),)),
            pltpu.SemaphoreType.DMA((4,)),
            pltpu.SemaphoreType.DMA((5,)),
            pltpu.SemaphoreType.DMA((5,)),
            pltpu.SemaphoreType.DMA,
            pltpu.SemaphoreType.DMA,
            pltpu.SemaphoreType.DMA((2,)),
            pltpu.SemaphoreType.DMA((2,)),
        ],
        compiler_params=pltpu.CompilerParams(
            collective_id=0, has_side_effects=True, vmem_limit_bytes=40 * 2**20
        ),
    )(
        timestep,
        *(
            pltpu.with_memory_space_constraint(tensor, pltpu.HBM)
            for tensor in (
                lengths,
                gate_table,
                video_self,
                video_far,
                video_far_halves,
                heads_inside(audio_qkv),
                heads_inside(audio_cross),
            )
        ),
    )
    return (
        video_out.reshape(clip_count, head_count, video_rows, head_size),
        jnp.swapaxes(audio_out, 1, 2),
    )


def solution(mesh):
    tokens = P("groups", None, None, "seq", None)
    made = P("groups", None, "seq", None)
    return jax.shard_map(
        on_device,
        mesh=mesh,
        in_specs=(tokens, tokens, tokens, tokens, P(None, "groups"), P("groups"), P()),
        out_specs=(made, made),
        check_vma=False,
    )
```
